256 devices in a mesh: rows: 32 (over x, z_lo, core), cols: 8 (over y, z_hi).
Axes of the slice: x: 4, y: 4, z: 8 (z_hi: 2, z_lo: 4; z = z_hi * 4 + z_lo), core: 2. Of those that a mesh axis runs over, the one named last changes fastest.
Arguments:
- image: float32 [2048, 16384], P('rows', 'cols'), may hold values from -6 to 6
- cloud_mask: int32 [2048, 16384], P('rows', 'cols'), may hold values 0 or 1
- tile_weight: int32 [256, 128], P('rows', 'cols'), may hold values from 1 to 8
- owner: int32 [256], replicated, may hold values from 0 to 31, as said below
Outputs:
- solution: float32 [2048, 16384], P('rows', 'cols')
- objective: float32 [3], replicated
The draws below stay inside these ranges and needn't reach their ends.
Inputs may be any that keep to these rules, and one draw needn't show every extreme that they name: `owner`: every index of rows owns exactly 8 blocks, and the 8 blocks b*8 to b*8 + 7 have 8 different owners for every b.
All inputs are finite; a program needn't handle non-finite values. No bound on the sum of `cloud_mask` on one device may be relied on, other than what follows from the above.
Results may differ from the reference program's by a relative error of at most 0.0001.
Values sent between devices are 32-bit elements; how exact they have to be, the bound alone decides.
No kernel may reach another device: no remote copies, remote signals or barrier semaphores. Data moves between devices by JAX's collectives and lax.ppermute only.
A program may use at most 64 MiB of HBM per device.

```python
import jax
import jax.numpy as jnp

BR = 8
BPD = 8
W = 16384
TW = 128
ITERS = 3
NBLK = 256
H = 2048
N_ROWS = 32


def draw_owner(key, part):
    folded = jax.random.fold_in(key, 11)
    shuffled = jax.random.permutation(jax.random.fold_in(folded, 1), N_ROWS).astype(jnp.int32)
    ranks = jnp.argsort(shuffled).astype(jnp.int32)
    values = jnp.arange(N_ROWS, dtype=jnp.int32)
    special = ((values == 1) | (values == N_ROWS // 2)).astype(jnp.int32)
    scores = ranks - 2 * N_ROWS * special
    offsets = jnp.argsort(scores).astype(jnp.int32)[:BPD]
    subkeys = jax.random.split(jax.random.fold_in(folded, 2), N_ROWS)
    orders = jax.vmap(lambda sub_key: jax.random.permutation(sub_key, BPD))(subkeys)
    source = jnp.arange(N_ROWS, dtype=jnp.int32)[:, None]
    owners = (source + offsets[orders]) % N_ROWS
    return owners.reshape(-1).astype(jnp.int32)


def set_ends(values, rng, smallest, largest):
    place = [jax.random.randint(jax.random.fold_in(rng, axis), (), 0, length) for axis, length in enumerate(values.shape)]
    longest = values.shape.index(max(values.shape))
    neighbour = place[:longest] + [(place[longest] + 1) % values.shape[longest]] + place[longest + 1:]
    return values.at[tuple(place)].set(smallest).at[tuple(neighbour)].set(largest)


def block_scale(key, extent, pieces, smallest, largest):
    gain = 1.0
    for axis_at, blocks in pieces:
        draws = jax.random.uniform(jax.random.fold_in(jax.random.fold_in(key, 6), axis_at), (blocks,), jnp.float32, smallest / len(pieces), largest / len(pieces))
        gain = gain * jnp.repeat(jnp.exp(draws), extent[axis_at] // blocks).reshape((-1,) + (1,) * (len(extent) - 1 - axis_at))
    return gain


def noise(own_key, dims, deviation, limit, cuts=(), kind=jnp.bfloat16):
    result = deviation * jax.random.normal(own_key, dims, jnp.float32)
    if cuts:
        result = result * block_scale(own_key, dims, cuts, -0.22, 0.18)
    return jnp.clip(result, -limit, limit).astype(kind)


def setup_inputs(seed: int = 0) -> dict:
    key_of = jax.random.split(jax.random.key(seed), 5)
    return {
        "image": noise(key_of[0], (H, W), 1.0, 6.0, ((0, 32), (1, 8)), jnp.float32),
        "cloud_mask": set_ends((jax.random.randint(key_of[1], (H, W), 0, 3) < 1).astype(jnp.int32), jax.random.fold_in(key_of[1], 1), 0, 1),
        "tile_weight": set_ends(jax.random.randint(key_of[2], (NBLK, W // TW), 1, 9), jax.random.fold_in(key_of[2], 1), 1, 8).astype(jnp.int32),
        "owner": draw_owner(jax.random.fold_in(key_of[4], 71), 0),
    }


fidelity_scale = 0.25
tau_step = 0.35
sigma_step = 0.35
tv_weight = 0.3

def forward_rows(field):
    return jnp.concatenate([field[1:] - field[:-1], jnp.zeros_like(field[:1])], axis=0)

def forward_cols(field):
    return jnp.concatenate([field[:, 1:] - field[:, :-1], jnp.zeros_like(field[:, :1])], axis=1)

def divergence(dual_rows, dual_cols):
    above = jnp.concatenate([jnp.zeros_like(dual_rows[:1]), dual_rows[:-1]], axis=0)
    leftward = jnp.concatenate([jnp.zeros_like(dual_cols[:, :1]), dual_cols[:, :-1]], axis=1)
    return dual_rows - above + (dual_cols - leftward)

def reference(image, cloud_mask, tile_weight, owner):
    height, width = image.shape
    total_blocks = owner.shape[0]
    tile_count = tile_weight.shape[1]
    per_tile = jnp.broadcast_to(tile_weight.astype(jnp.float32)[:, None, :, None], (total_blocks, BR, tile_count, TW)).reshape(height, width)
    fidelity = fidelity_scale * per_tile * (1 - cloud_mask).astype(jnp.float32)
    primal = image
    extrap = image
    dual_rows = jnp.zeros_like(image)
    dual_cols = jnp.zeros_like(image)
    objective_list = []
    for step in range(ITERS):
        grad_r = forward_rows(extrap)
        grad_c = forward_cols(extrap)
        trial_rows = dual_rows + sigma_step * grad_r
        trial_cols = dual_cols + sigma_step * grad_c
        shrink = jnp.maximum(1.0, jnp.sqrt(trial_rows * trial_rows + trial_cols * trial_cols) / tv_weight)
        dual_rows = trial_rows / shrink
        dual_cols = trial_cols / shrink
        updated = (primal + tau_step * divergence(dual_rows, dual_cols) + tau_step * fidelity * image) / (1.0 + tau_step * fidelity)
        misfit = updated - image
        total = jnp.sum(0.5 * fidelity * misfit * misfit) + tv_weight * jnp.sum(jnp.sqrt(grad_r * grad_r + grad_c * grad_c))
        objective_list.append(total / (height * width))
        extrap = 2.0 * updated - primal
        primal = updated
    order = jnp.argsort(owner, stable=True)
    solution = primal.reshape(total_blocks, BR, width)[order].reshape(height, width)
    return (solution, jnp.stack(objective_list).astype(jnp.float32))
```

```python
import functools

import jax
import jax.numpy as jnp
from jax import lax
from jax.experimental import pallas as pl
from jax.experimental.pallas import tpu as pltpu
from jax.sharding import PartitionSpec as P

BR = 8
TW = 128
ITERS = 3
HALF = TW // 2
PAD = 16
ROWS, COLS = "rows", "cols"

fidelity_scale = 0.25
tau_step = 0.35
sigma_step = 0.35
tv_weight = 0.3


def tile_fidelity(weight, mask):
    return (fidelity_scale * weight.astype(jnp.float32)) * (1 - mask).astype(jnp.float32)


def edges_kernel(tiles, weight, top, bottom, left, right, top_m, bottom_m, left_m, right_m, up, down, to_left, to_right, ul, ur, dl, dr):
    blocks = left.shape[0] // BR
    lane = lax.broadcasted_iota(jnp.int32, (BR, TW), 1)
    sub = lax.broadcasted_iota(jnp.int32, (BR, TW), 0)
    for t in range(tiles):
        cols = slice(t * TW, (t + 1) * TW)
        v = jnp.where(sub < 4, top[:, cols], pltpu.roll(tile_fidelity(weight[0, t], top_m[:, cols]), 4, 0))
        up[t] = v
        if t == 0:
            ul[...] = v
        if t == tiles - 1:
            ur[...] = v
        v = jnp.where(
            sub < 4, pltpu.roll(bottom[:, cols], 4, 0), tile_fidelity(weight[blocks - 1, t], bottom_m[:, cols])
        )
        down[t] = v
        if t == 0:
            dl[...] = v
        if t == tiles - 1:
            dr[...] = v
    for b in range(blocks):
        rows = slice(b * BR, (b + 1) * BR)
        f = tile_fidelity(weight[b, 0], left_m[rows])
        to_left[rows] = jnp.where(lane < HALF, left[rows], pltpu.roll(f, HALF, 1))
        f = tile_fidelity(weight[b, tiles - 1], right_m[rows])
        to_right[rows] = jnp.where(lane < HALF, pltpu.roll(f, HALF, 1), right[rows])


def edges(image, mask, weight):
    rows, width = image.shape
    tiles = width // TW
    last, side = rows // BR - 1, tiles - 1
    picked = [
        pl.BlockSpec((BR, width), lambda i: (0, 0)),
        pl.BlockSpec((BR, width), lambda i: (last, 0)),
        pl.BlockSpec((rows, TW), lambda i: (0, 0)),
        pl.BlockSpec((rows, TW), lambda i: (0, side)),
    ]
    shapes = [(tiles, BR, TW)] * 2 + [(rows, TW)] * 2 + [(BR, TW)] * 4
    return pl.pallas_call(
        functools.partial(edges_kernel, tiles),
        grid=(1,),
        in_specs=[pl.BlockSpec(memory_space=pltpu.SMEM)] + picked + picked,
        out_specs=[pl.BlockSpec(s, lambda i, n=len(s): (0,) * n) for s in shapes],
        out_shape=[jax.ShapeDtypeStruct(s, jnp.float32) for s in shapes],
        name="edges",
    )(weight, image, image, image, image, mask, mask, mask, mask)


def solve_kernel(
    tiles, blocks, height, width,
    where_, owner, weight, image, mask, below, above, from_right, from_left, br, bl, ar, al,
    slots, partial,
    img, msk, fid, inv, con, ext, pri, dual_r, dual_c, staged, in_sem, out_sem,
):
    rows = blocks * BR
    own_row, own_col = where_[0], where_[1]
    lane = lax.broadcasted_iota(jnp.int32, (BR, TW), 1)
    sub = lax.broadcasted_iota(jnp.int32, (BR, TW), 0)

    copies = []
    for t in range(tiles):
        cols = pl.ds(t * TW, TW)
        a = pltpu.make_async_copy(image.at[:, cols], img.at[t, pl.ds(PAD, rows)], in_sem.at[0, t])
        b = pltpu.make_async_copy(mask.at[:, cols], msk.at[t], in_sem.at[1, t])
        a.start()
        b.start()
        copies.append((a, b))

    def derive(t, at, f, g):
        fid[t, at] = f
        i = 1.0 / (1.0 + tau_step * f)
        inv[t, at] = i
        con[t, at] = (tau_step * f * g) * i

    low, high = slice(PAD - BR, PAD), slice(PAD + rows, PAD + rows + BR)
    for t in range(tiles + 1):
        if t < tiles:
            v, w = above[t], below[t]
        else:
            v = jnp.where(lane < HALF, ar[...], al[...])
            w = jnp.where(lane < HALF, br[...], bl[...])
        g = jnp.where(sub >= 4, pltpu.roll(v, 4, 0), 0.0)
        img[t, low] = g
        derive(t, low, jnp.where(sub >= 4, v, 0.0), g)
        g = jnp.where(sub < 4, w, 0.0)
        img[t, high] = g
        derive(t, high, jnp.where(sub < 4, pltpu.roll(w, 4, 0), 0.0), g)
    for b in range(blocks):
        at = slice(b * BR, (b + 1) * BR)
        here = slice(PAD + b * BR, PAD + (b + 1) * BR)
        r, l = from_right[at], from_left[at]
        g = jnp.where(lane < HALF, r, l)
        img[tiles, here] = g
        derive(tiles, here, pltpu.roll(jnp.where(lane < HALF, l, r), HALF, 1), g)
    for t in range(tiles):
        copies[t][0].wait()
        copies[t][1].wait()
        for b in range(blocks):
            here = slice(PAD + b * BR, PAD + (b + 1) * BR)
            derive(t, here, tile_fidelity(weight[b, t], msk[t, b * BR:(b + 1) * BR]), img[t, here])

    col = own_col * (tiles * TW) + lane
    inner_last = col + (tiles - 1) * TW < width - 1
    halo_col = jnp.where(lane < HALF, col + tiles * TW, col - TW)
    inner_halo = (halo_col >= 0) & (halo_col < width - 1)

    def sweep(k, r, acc, count):
        base = PAD - BR + r * BR
        if not isinstance(r, int):
            base = pl.multiple_of(base, BR)
        here, lower, upper = pl.ds(base, BR), pl.ds(base + 1, BR), pl.ds(base - 1, BR)
        first, final = k == 0, k == ITERS - 1
        source = img if first else ext
        row = own_row * rows + (r - 1) * BR + sub
        inner_row = (row >= 0) & (row < height - 1)

        def duals(t, e, right):
            g_r = jnp.where(inner_row, source[t, lower] - e, 0.0)
            g_c = right - e
            if t == tiles - 1:
                g_c = jnp.where(inner_last, g_c, 0.0)
            if t == tiles:
                g_c = jnp.where(inner_halo, g_c, 0.0)
            q_r, q_c = sigma_step * g_r, sigma_step * g_c
            if not first:
                q_r, q_c = dual_r[t, here] + q_r, dual_c[t, here] + q_c
            scale = jnp.minimum(1.0, tv_weight * lax.rsqrt(q_r * q_r + q_c * q_c))
            d_r, d_c = q_r * scale, q_c * scale
            dual_r[t, here] = d_r
            if not final:
                dual_c[t, here] = d_c
            return g_r, g_c, d_r, d_c

        def update(t, e, d_r, d_c, left):
            div = d_r - dual_r[t, upper] + (d_c - left)
            p = e if first else pri[t, here]
            u = (p + tau_step * div) * inv[t, here] + con[t, here]
            if final:
                if t < tiles and count:
                    staged[r - 1, :, t * TW:(t + 1) * TW] = u
            else:
                ext[t, here] = 2.0 * u - p
                pri[t, here] = u
            return u

        e_halo = source[tiles, here]
        e = source[0, here]
        turned = pltpu.roll(e, TW - 1, 1)
        turned_halo = pltpu.roll(e_halo, TW - 1, 1)
        _, _, h_r, h_c = duals(tiles, e_halo, jnp.where(lane == TW - 1, turned, turned_halo))
        shifted = pltpu.roll(h_c, 1, 1)
        shifted_halo = shifted
        fit, tv = acc
        for t in range(tiles):
            if t < tiles - 1:
                e_next = source[t + 1, here]
                turned_next = pltpu.roll(e_next, TW - 1, 1)
            else:
                e_next, turned_next = None, turned_halo
            g_r, g_c, d_r, d_c = duals(t, e, jnp.where(lane == TW - 1, turned_next, turned))
            shifted_here = pltpu.roll(d_c, 1, 1)
            u = update(t, e, d_r, d_c, jnp.where(lane == 0, shifted, shifted_here))
            if count:
                miss = u - img[t, here]
                fit = fit + fid[t, here] * (miss * miss)
                tv = tv + jnp.sqrt(g_r * g_r + g_c * g_c)
            shifted, e, turned = shifted_here, e_next, turned_next
        if not final:
            update(tiles, e_halo, h_r, h_c, jnp.where(lane == 0, shifted, shifted_halo))
        return fit, tv

    def send(b):
        return pltpu.make_async_copy(staged.at[b], slots.at[owner[own_row * blocks + b]], out_sem.at[b])

    zero = jnp.zeros((BR, TW), jnp.float32)
    total = zero
    for k in range(ITERS):
        sweep(k, 0, (zero, zero), False)

        def body(r, acc, k=k):
            acc = sweep(k, r, acc, True)
            if k == ITERS - 1:

                @pl.when(r >= 2)
                def _():
                    send(r - 2).start()

            return acc

        fit, tv = lax.fori_loop(1, blocks + 1, body, (zero, zero))
        if k < ITERS - 1:
            sweep(k, blocks + 1, (zero, zero), False)
        total = jnp.where(lane == k, jnp.sum(0.5 * fit + tv_weight * tv), total)
    send(blocks - 1).start()
    partial[...] = total
    for b in range(blocks):
        send(b).wait()


def solve(where_, owner, weight, image, mask, halos, row_count, height, width):
    rows, here = image.shape
    blocks, tiles = rows // BR, here // TW
    deep = pltpu.VMEM((tiles + 1, PAD + rows + PAD, TW), jnp.float32)
    smem, vmem, anywhere = (pl.BlockSpec(memory_space=s) for s in (pltpu.SMEM, pltpu.VMEM, pl.ANY))
    return pl.pallas_call(
        functools.partial(solve_kernel, tiles, blocks, height, width),
        in_specs=[smem] * 3 + [anywhere] * 2 + [vmem] * 8,
        out_specs=[anywhere, vmem],
        out_shape=[
            jax.ShapeDtypeStruct((row_count, BR, here), jnp.float32),
            jax.ShapeDtypeStruct((BR, TW), jnp.float32),
        ],
        scratch_shapes=[
            deep,
            pltpu.VMEM((tiles, rows, TW), jnp.int32),
            deep, deep, deep, deep, deep, deep, deep,
            pltpu.VMEM((blocks, BR, here), jnp.float32),
            pltpu.SemaphoreType.DMA((2, tiles)),
            pltpu.SemaphoreType.DMA((blocks,)),
        ],
        compiler_params=pltpu.CompilerParams(vmem_limit_bytes=24 * 2**20),
        name="solve",
    )(where_, owner, weight, image, mask, *halos)


def lookup_kernel(blocks, where_, owner, senders):
    def body(b, found):
        mine = owner[b] == where_[0]

        @pl.when(mine)
        def _():
            senders[found] = b // blocks

        return found + mine.astype(jnp.int32)

    lax.fori_loop(0, owner.shape[0], body, jnp.int32(0))


def place_kernel(senders, slot, out):
    out[...] = slot[0]


def per_device(image, cloud_mask, tile_weight, owner):
    rows_here, width_here = image.shape
    blocks = rows_here // BR
    row_count, col_count = lax.axis_size(ROWS), lax.axis_size(COLS)
    height, width = rows_here * row_count, width_here * col_count
    own_row, own_col = lax.axis_index(ROWS), lax.axis_index(COLS)
    where_ = jnp.stack([own_row, own_col]).astype(jnp.int32)

    def moved(array, down, right):
        route = [
            (r * col_count + c, (r + down) * col_count + c + right)
            for r in range(row_count)
            for c in range(col_count)
            if 0 <= r + down < row_count and 0 <= c + right < col_count
        ]
        return lax.ppermute(array, (ROWS, COLS), route)

    up, down, to_left, to_right, ul, ur, dl, dr = edges(image, cloud_mask, tile_weight)
    halos = (
        moved(up, -1, 0), moved(down, 1, 0), moved(to_left, 0, -1), moved(to_right, 0, 1),
        moved(ul, -1, -1), moved(ur, -1, 1), moved(dl, 1, -1), moved(dr, 1, 1),
    )
    slots, partial = solve(where_, owner, tile_weight, image, cloud_mask, halos, row_count, height, width)
    arrived = lax.all_to_all(slots, ROWS, split_axis=0, concat_axis=0, tiled=True)

    smem = pl.BlockSpec(memory_space=pltpu.SMEM)
    senders = pl.pallas_call(
        functools.partial(lookup_kernel, blocks),
        in_specs=[smem, smem],
        out_specs=smem,
        out_shape=jax.ShapeDtypeStruct((blocks,), jnp.int32),
        name="lookup",
    )(where_, owner)

    total = partial[:1]
    devices = row_count * col_count
    step = 1
    while step < devices:
        total = total + lax.ppermute(total, (ROWS, COLS), [(i, i ^ step) for i in range(devices)])
        step *= 2
    objective = total[0, :ITERS] / (height * width)

    solution = pl.pallas_call(
        place_kernel,
        grid_spec=pltpu.PrefetchScalarGridSpec(
            num_scalar_prefetch=1,
            grid=(blocks,),
            in_specs=[pl.BlockSpec((1, BR, width_here), lambda k, senders: (senders[k], 0, 0))],
            out_specs=pl.BlockSpec((BR, width_here), lambda k, senders: (k, 0)),
        ),
        out_shape=jax.ShapeDtypeStruct((rows_here, width_here), jnp.float32),
        name="place",
    )(senders, arrived)
    return solution, objective


def solution(mesh):
    placed = (P(ROWS, COLS), P(ROWS, COLS), P(ROWS, COLS), P())
    return jax.shard_map(per_device, mesh=mesh, in_specs=placed, out_specs=(P(ROWS, COLS), P()), check_vma=False)
```

```python
import functools

import jax
import jax.numpy as jnp
from jax import lax
from jax.experimental import pallas as pl
from jax.experimental.pallas import tpu as pltpu
from jax.sharding import PartitionSpec as P

BR = 8
TW = 128
ITERS = 3
HALF = TW // 2
PAD = 16
ROWS, COLS = "rows", "cols"
ALONG_Z = (1, 16, 32)

fidelity_scale = 0.25
tau_step = 0.35
sigma_step = 0.35
tv_weight = 0.3


def vmem_grant(mebibytes):
    return pltpu.CompilerParams(vmem_limit_bytes=mebibytes * 2**20)


def tile_fidelity(weight, mask):
    return (tau_step * fidelity_scale * weight.astype(jnp.float32)) * (1 - mask).astype(jnp.float32)


def sides_kernel(tiles, weight, image, mask, to_left, to_right, img, msk, sem):
    lane = lax.broadcasted_iota(jnp.int32, (BR, TW), 1)
    copies = [
        pltpu.make_async_copy(source.at[:, pl.ds(t * TW, TW)], kept.at[side], sem.at[2 * side + i])
        for side, t in enumerate((0, tiles - 1))
        for i, (source, kept) in enumerate(((image, img), (mask, msk)))
    ]
    for copy in copies:
        copy.start()
    for copy in copies:
        copy.wait()
    for b in range(image.shape[0] // BR):
        rows = slice(b * BR, (b + 1) * BR)
        f = tile_fidelity(weight[b, 0], msk[0, rows])
        to_left[rows] = jnp.where(lane < HALF, img[0, rows], pltpu.roll(f, HALF, 1))
        f = tile_fidelity(weight[b, tiles - 1], msk[1, rows])
        to_right[rows] = jnp.where(lane < HALF, pltpu.roll(f, HALF, 1), img[1, rows])


def prep_kernel(tiles, blocks, weight, image, mask, img, fid, inv, up, down):
    sub = lax.broadcasted_iota(jnp.int32, (BR, TW), 0)
    for t in range(tiles):
        for b in range(blocks):
            rows, cols = slice(b * BR, (b + 1) * BR), slice(t * TW, (t + 1) * TW)
            here = slice(PAD + b * BR, PAD + (b + 1) * BR)
            g, f = image[rows, cols], tile_fidelity(weight[b, t], mask[rows, cols])
            img[t, here] = g
            fid[t, here] = f
            inv[t, here] = 1.0 / (1.0 + f)
            if b == 0:
                up[t] = jnp.where(sub < 4, g, pltpu.roll(f, 4, 0))
            if b == blocks - 1:
                down[t] = jnp.where(sub < 4, pltpu.roll(g, 4, 0), f)


def halo_tile(from_right, from_left, rows):
    lane = lax.broadcasted_iota(jnp.int32, (BR, TW), 1)
    r, l = from_right[rows], from_left[rows]
    return jnp.where(lane < HALF, r, l), pltpu.roll(jnp.where(lane < HALF, l, r), HALF, 1)


def corners_kernel(tiles, from_right, from_left, up_in, down_in, up, down):
    rows = from_right.shape[0]
    sub = lax.broadcasted_iota(jnp.int32, (BR, TW), 0)
    g, f = halo_tile(from_right, from_left, slice(0, BR))
    up[tiles] = jnp.where(sub < 4, g, pltpu.roll(f, 4, 0))
    g, f = halo_tile(from_right, from_left, slice(rows - BR, rows))
    down[tiles] = jnp.where(sub < 4, pltpu.roll(g, 4, 0), f)


def solve_kernel(
    tiles, blocks, height, width,
    where_, owner, senders, below, above, from_right, from_left, img_in, fid_in, inv_in,
    slots, partial, img, fid, inv,
    ext, pri, dual_r, dual_c, staged, sem,
):
    rows = blocks * BR
    own_row, own_col = where_[0], where_[1]
    lane = lax.broadcasted_iota(jnp.int32, (BR, TW), 1)
    sub = lax.broadcasted_iota(jnp.int32, (BR, TW), 0)

    low, high = slice(PAD - BR, PAD), slice(PAD + rows, PAD + rows + BR)
    for t in range(tiles + 1):
        v, w = above[t], below[t]
        for at, g, f in (
            (low, jnp.where(sub >= 4, pltpu.roll(v, 4, 0), 0.0), jnp.where(sub >= 4, v, 0.0)),
            (high, jnp.where(sub < 4, w, 0.0), jnp.where(sub < 4, pltpu.roll(w, 4, 0), 0.0)),
        ):
            img[t, at] = g
            fid[t, at] = f
            inv[t, at] = 1.0 / (1.0 + f)
    for b in range(blocks):
        here = slice(PAD + b * BR, PAD + (b + 1) * BR)
        g, f = halo_tile(from_right, from_left, slice(b * BR, (b + 1) * BR))
        img[tiles, here] = g
        fid[tiles, here] = f
        inv[tiles, here] = 1.0 / (1.0 + f)

    col = own_col * (tiles * TW) + lane
    inner_last = col + (tiles - 1) * TW < width - 1
    halo_col = jnp.where(lane < HALF, col + tiles * TW, col - TW)
    inner_halo = (halo_col >= 0) & (halo_col < width - 1)

    def send(b):
        return pltpu.make_async_copy(staged.at[b], slots.at[owner[own_row * blocks + b]], sem.at[b])

    def sweep(k, r, acc):
        base = pl.multiple_of(PAD - BR + r * BR, BR)
        here, lower, upper = pl.ds(base, BR), pl.ds(base + 1, BR), pl.ds(base - 1, BR)
        first, final = k == 0, k == ITERS - 1
        source = img if first else ext
        row = own_row * rows + (r - 1) * BR + sub
        inner_row = (row >= 0) & (row < height - 1)
        block = jnp.maximum(r - 1, 0)

        def duals(t, e, right):
            g_r = jnp.where(inner_row, source[t, lower] - e, 0.0)
            g_c = right - e
            if t == tiles - 1:
                g_c = jnp.where(inner_last, g_c, 0.0)
            if t == tiles:
                g_c = jnp.where(inner_halo, g_c, 0.0)
            n = g_r * g_r + g_c * g_c
            s = lax.rsqrt(n)
            steep = jnp.where(n > 0.0, n * s, 0.0)
            q_r, q_c = g_r, g_c
            if not first:
                q_r, q_c = dual_r[t, here] + q_r, dual_c[t, here] + q_c
                s = lax.rsqrt(q_r * q_r + q_c * q_c)
            scale = jnp.minimum(1.0, (tv_weight / sigma_step) * s)
            d_r, d_c = q_r * scale, q_c * scale
            dual_r[t, here] = d_r
            if not final:
                dual_c[t, here] = d_c
            return steep, d_r, d_c

        def update(t, e, d_r, d_c, left, pull):
            div = d_r - dual_r[t, upper] + (d_c - left)
            p = e if first else pri[t, here]
            u = (p + (tau_step * sigma_step) * div + pull) * inv[t, here]
            if final:
                if t < tiles:
                    staged[block, :, t * TW:(t + 1) * TW] = u
            else:
                ext[t, here] = u + (u - p)
                pri[t, here] = u
            return u

        e_halo = source[tiles, here]
        e = source[0, here]
        turned = pltpu.roll(e, TW - 1, 1)
        turned_halo = pltpu.roll(e_halo, TW - 1, 1)
        _, h_r, h_c = duals(tiles, e_halo, jnp.where(lane == TW - 1, turned, turned_halo))
        shifted = pltpu.roll(h_c, 1, 1)
        shifted_halo = shifted
        fit, tv = acc
        for t in range(tiles):
            if t < tiles - 1:
                e_next = source[t + 1, here]
                turned_next = pltpu.roll(e_next, TW - 1, 1)
            else:
                e_next, turned_next = None, turned_halo
            steep, d_r, d_c = duals(t, e, jnp.where(lane == TW - 1, turned_next, turned))
            shifted_here = pltpu.roll(d_c, 1, 1)
            g, f = img[t, here], fid[t, here]
            u = update(t, e, d_r, d_c, jnp.where(lane == 0, shifted, shifted_here), f * g)
            miss = u - g
            fit = fit + f * (miss * miss)
            tv = tv + steep
            shifted, e, turned = shifted_here, e_next, turned_next
        if not final:
            update(tiles, e_halo, h_r, h_c, jnp.where(lane == 0, shifted, shifted_halo), fid[tiles, here] * img[tiles, here])
        if final:

            @pl.when(r >= 2)
            def _():
                send(r - 2).start()

        own = jnp.logical_and(r >= 1, r <= blocks)
        return jnp.where(own, fit, acc[0]), jnp.where(own, tv, acc[1])

    zero = jnp.zeros((BR, TW), jnp.float32)
    total = zero
    for k in range(ITERS):
        last = blocks + 2 if k < ITERS - 1 else blocks + 1
        fit, tv = lax.fori_loop(0, last, functools.partial(sweep, k), (zero, zero))
        total = jnp.where(lane == k, jnp.sum((0.5 / tau_step) * fit + tv_weight * tv), total)
    send(blocks - 1).start()
    partial[...] = total
    for b in range(blocks):
        send(b).wait()


def lookup_kernel(blocks, where_, owner, senders):
    def body(b, found):
        mine = owner[b] == where_[0]

        @pl.when(mine)
        def _():
            senders[found] = b // blocks

        return found + mine.astype(jnp.int32)

    lax.fori_loop(0, owner.shape[0], body, jnp.int32(0))


def place_kernel(blocks, senders, arrived, out, sem):
    copies = [
        pltpu.make_async_copy(arrived.at[senders[k]], out.at[pl.ds(k * BR, BR)], sem.at[k]) for k in range(blocks)
    ]
    for copy in copies:
        copy.start()
    for copy in copies:
        copy.wait()


def per_device(image, cloud_mask, tile_weight, owner):
    rows_here, width_here = image.shape
    blocks, tiles = rows_here // BR, width_here // TW
    row_count, col_count = lax.axis_size(ROWS), lax.axis_size(COLS)
    height, width = rows_here * row_count, width_here * col_count
    own_row, own_col = lax.axis_index(ROWS), lax.axis_index(COLS)
    where_ = jnp.stack([own_row, own_col]).astype(jnp.int32)
    smem, vmem, hbm, anywhere = (pl.BlockSpec(memory_space=s) for s in (pltpu.SMEM, pltpu.VMEM, pltpu.HBM, pl.ANY))

    def shape(*dims):
        return jax.ShapeDtypeStruct(dims, jnp.float32)

    def work(flops):
        return pl.CostEstimate(flops=flops, bytes_accessed=0, transcendentals=0)

    def moved(array, axis, distance):
        size = lax.axis_size(axis)
        return lax.ppermute(array, axis, [(i, i + distance) for i in range(size) if 0 <= i + distance < size])

    to_left, to_right = pl.pallas_call(
        functools.partial(sides_kernel, tiles),
        in_specs=[smem, hbm, hbm],
        out_specs=[vmem] * 2,
        out_shape=[shape(rows_here, TW)] * 2,
        scratch_shapes=[
            pltpu.VMEM((2, rows_here, TW), jnp.float32),
            pltpu.VMEM((2, rows_here, TW), jnp.int32),
            pltpu.SemaphoreType.DMA((4,)),
        ],
        name="sides",
    )(tile_weight, image, cloud_mask)
    from_right, from_left = moved(to_left, COLS, -1), moved(to_right, COLS, 1)
    deep, edge = shape(tiles + 1, PAD + rows_here + PAD, TW), shape(tiles + 1, BR, TW)
    *fields, up, down = pl.pallas_call(
        functools.partial(prep_kernel, tiles, blocks),
        in_specs=[smem, vmem, vmem],
        out_specs=[vmem] * 5,
        out_shape=[deep] * 3 + [edge] * 2,
        cost_estimate=work(2 * 10**9),
        compiler_params=vmem_grant(16),
        name="prep",
    )(tile_weight, image, cloud_mask)
    up, down = pl.pallas_call(
        functools.partial(corners_kernel, tiles),
        in_specs=[vmem] * 4,
        out_specs=[vmem] * 2,
        out_shape=[edge] * 2,
        input_output_aliases={2: 0, 3: 1},
        compiler_params=vmem_grant(2),
        name="corners",
    )(from_right, from_left, up, down)
    below, above = moved(up, ROWS, -1), moved(down, ROWS, 1)
    senders = pl.pallas_call(
        functools.partial(lookup_kernel, blocks),
        in_specs=[smem, smem],
        out_specs=smem,
        out_shape=jax.ShapeDtypeStruct((blocks,), jnp.int32),
        cost_estimate=work(2 * 10**9),
        compiler_params=vmem_grant(1),
        name="lookup",
    )(where_, owner)
    slots, partial, *_ = pl.pallas_call(
        functools.partial(solve_kernel, tiles, blocks, height, width),
        in_specs=[smem] * 3 + [vmem] * 7,
        out_specs=[hbm] + [vmem] * 4,
        out_shape=[shape(row_count, BR, width_here), shape(BR, TW)] + [deep] * 3,
        input_output_aliases={7: 2, 8: 3, 9: 4},
        scratch_shapes=[pltpu.VMEM(deep.shape, jnp.float32)] * 4
        + [pltpu.VMEM((blocks, BR, width_here), jnp.float32), pltpu.SemaphoreType.DMA((blocks,))],
        compiler_params=vmem_grant(51),
        name="solve",
    )(where_, owner, senders, below, above, from_right, from_left, *fields)
    arrived = lax.all_to_all(slots, ROWS, split_axis=0, concat_axis=0, tiled=True)

    total = partial[:1]
    devices = row_count * col_count
    bits = [1 << i for i in range(devices.bit_length() - 1)]
    bits.sort(key=lambda bit: bit in ALONG_Z)
    for bit in bits:
        total = total + lax.ppermute(total, (ROWS, COLS), [(i, i ^ bit) for i in range(devices)])
    objective = total[0, :ITERS] / (height * width)

    solution = pl.pallas_call(
        functools.partial(place_kernel, blocks),
        in_specs=[smem, anywhere],
        out_specs=anywhere,
        out_shape=shape(rows_here, width_here),
        scratch_shapes=[pltpu.SemaphoreType.DMA((blocks,))],
        compiler_params=vmem_grant(1),
        name="place",
    )(senders, arrived)
    return solution, objective


def solution(mesh):
    placed = (P(ROWS, COLS), P(ROWS, COLS), P(ROWS, COLS), P())
    return jax.shard_map(per_device, mesh=mesh, in_specs=placed, out_specs=(P(ROWS, COLS), P()), check_vma=False)
```

```python
import functools

import jax
import jax.numpy as jnp
from jax import lax
from jax.experimental import pallas as pl
from jax.experimental.pallas import tpu as pltpu
from jax.sharding import PartitionSpec as P

BR = 8
TW = 128
ITERS = 3
HALF = TW // 2
PAD = 16
ROWS, COLS = "rows", "cols"
ALONG_Z = (1, 16, 32)

fidelity_scale = 0.25
tau_step = 0.35
sigma_step = 0.35
tv_weight = 0.3


def vmem_grant(mebibytes):
    return pltpu.CompilerParams(vmem_limit_bytes=int(mebibytes * 2**20))


def tile_fidelity(weight, mask):
    return (tau_step * fidelity_scale * weight.astype(jnp.float32)) * (1 - mask).astype(jnp.float32)


def sides_kernel(tiles, weight, image, mask, to_left, to_right, up, down, img, msk, img_rows, msk_rows, sem):
    rows = image.shape[0]
    blocks = rows // BR
    lane = lax.broadcasted_iota(jnp.int32, (BR, TW), 1)
    sub = lax.broadcasted_iota(jnp.int32, (BR, TW), 0)
    copies = []
    for side in range(2):
        column, row = pl.ds(side * (tiles - 1) * TW, TW), pl.ds(side * (rows - BR), BR)
        for source, kept, kept_rows in ((image, img, img_rows), (mask, msk, msk_rows)):
            copies.append(pltpu.make_async_copy(source.at[:, column], kept.at[side], sem.at[len(copies)]))
            copies.append(pltpu.make_async_copy(source.at[row], kept_rows.at[side], sem.at[len(copies)]))
    for copy in copies:
        copy.start()
    for copy in copies:
        copy.wait()
    for b in range(blocks):
        here = slice(b * BR, (b + 1) * BR)
        f = tile_fidelity(weight[b, 0], msk[0, here])
        to_left[here] = jnp.where(lane < HALF, img[0, here], pltpu.roll(f, HALF, 1))
        f = tile_fidelity(weight[b, tiles - 1], msk[1, here])
        to_right[here] = jnp.where(lane < HALF, pltpu.roll(f, HALF, 1), img[1, here])
    for t in range(tiles):
        cols = slice(t * TW, (t + 1) * TW)
        f = tile_fidelity(weight[0, t], msk_rows[0, :, cols])
        up[t] = jnp.where(sub < 4, img_rows[0, :, cols], pltpu.roll(f, 4, 0))
        f = tile_fidelity(weight[blocks - 1, t], msk_rows[1, :, cols])
        down[t] = jnp.where(sub < 4, pltpu.roll(img_rows[1, :, cols], 4, 0), f)


def halo_tile(from_right, from_left, rows):
    lane = lax.broadcasted_iota(jnp.int32, (BR, TW), 1)
    r, l = from_right[rows], from_left[rows]
    return jnp.where(lane < HALF, r, l), pltpu.roll(jnp.where(lane < HALF, l, r), HALF, 1)


def corners_kernel(tiles, from_right, from_left, up_in, down_in, up, down):
    rows = from_right.shape[0]
    sub = lax.broadcasted_iota(jnp.int32, (BR, TW), 0)
    for t in range(tiles):
        up[t], down[t] = up_in[t], down_in[t]
    g, f = halo_tile(from_right, from_left, slice(0, BR))
    up[tiles] = jnp.where(sub < 4, g, pltpu.roll(f, 4, 0))
    g, f = halo_tile(from_right, from_left, slice(rows - BR, rows))
    down[tiles] = jnp.where(sub < 4, pltpu.roll(g, 4, 0), f)


def solve_kernel(
    tiles, blocks, height, width,
    where_, owner, weight, image, mask, below, above, from_right, from_left,
    slots, partial,
    img, fid, inv, ext, pri, dual_r, dual_c, staged, sem,
):
    rows = blocks * BR
    own_row, own_col = where_[0], where_[1]
    lane = lax.broadcasted_iota(jnp.int32, (BR, TW), 1)
    sub = lax.broadcasted_iota(jnp.int32, (BR, TW), 0)

    for t in range(tiles):
        for b in range(blocks):
            natural, cols = slice(b * BR, (b + 1) * BR), slice(t * TW, (t + 1) * TW)
            here = slice(PAD + b * BR, PAD + (b + 1) * BR)
            f = tile_fidelity(weight[b, t], mask[natural, cols])
            img[t, here] = image[natural, cols]
            fid[t, here] = f
            inv[t, here] = 1.0 / (1.0 + f)
    low, high = slice(PAD - BR, PAD), slice(PAD + rows, PAD + rows + BR)
    for t in range(tiles + 1):
        v, w = above[t], below[t]
        for at, g, f in (
            (low, jnp.where(sub >= 4, pltpu.roll(v, 4, 0), 0.0), jnp.where(sub >= 4, v, 0.0)),
            (high, jnp.where(sub < 4, w, 0.0), jnp.where(sub < 4, pltpu.roll(w, 4, 0), 0.0)),
        ):
            img[t, at] = g
            fid[t, at] = f
            inv[t, at] = 1.0 / (1.0 + f)
    for b in range(blocks):
        here = slice(PAD + b * BR, PAD + (b + 1) * BR)
        g, f = halo_tile(from_right, from_left, slice(b * BR, (b + 1) * BR))
        img[tiles, here] = g
        fid[tiles, here] = f
        inv[tiles, here] = 1.0 / (1.0 + f)

    col = own_col * (tiles * TW) + lane
    inner_last = col + (tiles - 1) * TW < width - 1
    halo_col = jnp.where(lane < HALF, col + tiles * TW, col - TW)
    inner_halo = (halo_col >= 0) & (halo_col < width - 1)

    def send(b):
        return pltpu.make_async_copy(staged.at[b], slots.at[owner[own_row * blocks + b]], sem.at[b])

    def sweep(k, r, acc):
        base = pl.multiple_of(PAD - BR + r * BR, BR)
        here, lower, upper = pl.ds(base, BR), pl.ds(base + 1, BR), pl.ds(base - 1, BR)
        first, final = k == 0, k == ITERS - 1
        source = img if first else ext
        row = own_row * rows + (r - 1) * BR + sub
        inner_row = (row >= 0) & (row < height - 1)
        block = jnp.maximum(r - 1, 0)

        def duals(t, e, right):
            g_r = jnp.where(inner_row, source[t, lower] - e, 0.0)
            g_c = right - e
            if t == tiles - 1:
                g_c = jnp.where(inner_last, g_c, 0.0)
            if t == tiles:
                g_c = jnp.where(inner_halo, g_c, 0.0)
            n = g_r * g_r + g_c * g_c
            s = lax.rsqrt(n)
            steep = jnp.where(n > 0.0, n * s, 0.0)
            q_r, q_c = g_r, g_c
            if not first:
                q_r, q_c = dual_r[t, here] + q_r, dual_c[t, here] + q_c
                s = lax.rsqrt(q_r * q_r + q_c * q_c)
            scale = jnp.minimum(1.0, (tv_weight / sigma_step) * s)
            d_r, d_c = q_r * scale, q_c * scale
            dual_r[t, here] = d_r
            if not final:
                dual_c[t, here] = d_c
            return steep, d_r, d_c

        def update(t, e, d_r, d_c, left, pull):
            div = d_r - dual_r[t, upper] + (d_c - left)
            p = e if first else pri[t, here]
            u = (p + (tau_step * sigma_step) * div + pull) * inv[t, here]
            if final:
                if t < tiles:
                    staged[block, :, t * TW:(t + 1) * TW] = u
            else:
                ext[t, here] = u + (u - p)
                pri[t, here] = u
            return u

        e_halo = source[tiles, here]
        e = source[0, here]
        turned = pltpu.roll(e, TW - 1, 1)
        turned_halo = pltpu.roll(e_halo, TW - 1, 1)
        _, h_r, h_c = duals(tiles, e_halo, jnp.where(lane == TW - 1, turned, turned_halo))
        shifted = pltpu.roll(h_c, 1, 1)
        shifted_halo = shifted
        fit, tv = acc
        for t in range(tiles):
            if t < tiles - 1:
                e_next = source[t + 1, here]
                turned_next = pltpu.roll(e_next, TW - 1, 1)
            else:
                e_next, turned_next = None, turned_halo
            steep, d_r, d_c = duals(t, e, jnp.where(lane == TW - 1, turned_next, turned))
            shifted_here = pltpu.roll(d_c, 1, 1)
            g, f = img[t, here], fid[t, here]
            u = update(t, e, d_r, d_c, jnp.where(lane == 0, shifted, shifted_here), f * g)
            miss = u - g
            fit = fit + f * (miss * miss)
            tv = tv + steep
            shifted, e, turned = shifted_here, e_next, turned_next
        if not final:
            update(tiles, e_halo, h_r, h_c, jnp.where(lane == 0, shifted, shifted_halo), fid[tiles, here] * img[tiles, here])
        if final:

            @pl.when(r >= 2)
            def _():
                send(r - 2).start()

        own = jnp.logical_and(r >= 1, r <= blocks)
        return jnp.where(own, fit, acc[0]), jnp.where(own, tv, acc[1])

    zero = jnp.zeros((BR, TW), jnp.float32)
    total = zero
    for k in range(ITERS):
        last = blocks + 2 if k < ITERS - 1 else blocks + 1
        fit, tv = lax.fori_loop(0, last, functools.partial(sweep, k), (zero, zero))
        total = jnp.where(lane == k, jnp.sum((0.5 / tau_step) * fit + tv_weight * tv), total)
    send(blocks - 1).start()
    partial[...] = total
    for b in range(blocks):
        send(b).wait()


def lookup_kernel(blocks, where_, owner, senders):
    def body(sender, found):
        mine = owner[sender * blocks] == where_[0]
        for i in range(1, blocks):
            mine |= owner[sender * blocks + i] == where_[0]
        senders[found] = sender
        return found + mine.astype(jnp.int32)

    lax.fori_loop(0, owner.shape[0] // blocks, body, jnp.int32(0))


def place_kernel(blocks, pixels, senders, arrived, *refs):
    parts, (out, objective, sem) = refs[:-3], refs[-3:]
    copies = [
        pltpu.make_async_copy(arrived.at[senders[k]], out.at[pl.ds(k * BR, BR)], sem.at[k]) for k in range(blocks)
    ]
    for copy in copies:
        copy.start()
    values = [part[...] for part in parts]
    while len(values) > 1:
        values = [a + b for a, b in zip(values[::2], values[1::2])]
    lane = lax.broadcasted_iota(jnp.int32, values[0].shape, 1)
    for k in range(ITERS):
        objective[k] = jnp.sum(jnp.where(lane == k, values[0], 0.0)) / pixels
    for copy in copies:
        copy.wait()


def per_device(image, cloud_mask, tile_weight, owner):
    rows_here, width_here = image.shape
    blocks, tiles = rows_here // BR, width_here // TW
    row_count, col_count = lax.axis_size(ROWS), lax.axis_size(COLS)
    height, width = rows_here * row_count, width_here * col_count
    own_row, own_col = lax.axis_index(ROWS), lax.axis_index(COLS)
    where_ = jnp.stack([own_row, own_col]).astype(jnp.int32)
    smem, vmem, hbm, anywhere = (pl.BlockSpec(memory_space=s) for s in (pltpu.SMEM, pltpu.VMEM, pltpu.HBM, pl.ANY))

    def shape(*dims):
        return jax.ShapeDtypeStruct(dims, jnp.float32)

    def work(flops):
        return pl.CostEstimate(flops=flops, bytes_accessed=0, transcendentals=0)

    def moved(array, axis, distance):
        size = lax.axis_size(axis)
        return lax.ppermute(array, axis, [(i, i + distance) for i in range(size) if 0 <= i + distance < size])

    edge = shape(tiles + 1, BR, TW)
    to_left, to_right, up, down = pl.pallas_call(
        functools.partial(sides_kernel, tiles),
        in_specs=[smem, hbm, hbm],
        out_specs=[vmem] * 4,
        out_shape=[shape(rows_here, TW)] * 2 + [edge] * 2,
        scratch_shapes=[
            pltpu.VMEM((2, rows_here, TW), jnp.float32),
            pltpu.VMEM((2, rows_here, TW), jnp.int32),
            pltpu.VMEM((2, BR, width_here), jnp.float32),
            pltpu.VMEM((2, BR, width_here), jnp.int32),
            pltpu.SemaphoreType.DMA((8,)),
        ],
        cost_estimate=work(2 * 10**9),
        compiler_params=vmem_grant(53.5),
        name="sides",
    )(tile_weight, image, cloud_mask)
    from_right, from_left = moved(to_left, COLS, -1), moved(to_right, COLS, 1)
    up, down = pl.pallas_call(
        functools.partial(corners_kernel, tiles),
        in_specs=[vmem] * 4,
        out_specs=[vmem] * 2,
        out_shape=[edge] * 2,
        cost_estimate=work(2 * 10**9),
        compiler_params=vmem_grant(2),
        name="corners",
    )(from_right, from_left, up, down)
    below, above = moved(up, ROWS, -1), moved(down, ROWS, 1)
    slots, partial = pl.pallas_call(
        functools.partial(solve_kernel, tiles, blocks, height, width),
        in_specs=[smem] * 3 + [vmem] * 6,
        out_specs=[hbm, vmem],
        out_shape=[shape(row_count, BR, width_here), shape(BR, TW)],
        scratch_shapes=[pltpu.VMEM((tiles + 1, PAD + rows_here + PAD, TW), jnp.float32)] * 7
        + [pltpu.VMEM((blocks, BR, width_here), jnp.float32), pltpu.SemaphoreType.DMA((blocks,))],
        compiler_params=vmem_grant(52),
        name="solve",
    )(where_, owner, tile_weight, image, cloud_mask, below, above, from_right, from_left)
    arrived = lax.all_to_all(slots, ROWS, split_axis=0, concat_axis=0, tiled=True)

    later, _ = lax.optimization_barrier((owner, partial))
    senders = pl.pallas_call(
        functools.partial(lookup_kernel, blocks),
        in_specs=[smem, smem],
        out_specs=smem,
        out_shape=jax.ShapeDtypeStruct((2 * blocks,), jnp.int32),
        compiler_params=vmem_grant(1),
        name="lookup",
    )(where_, later)

    devices = row_count * col_count

    def swapped(array, mask):
        return lax.ppermute(array, (ROWS, COLS), [(i, i ^ mask) for i in range(devices)])

    total = partial[:1]
    for bit in (1 << i for i in range(devices.bit_length() - 1)):
        if bit not in ALONG_Z:
            total = total + swapped(total, bit)
    masks = [0]
    for bit in ALONG_Z:
        masks += [mask | bit for mask in masks]
    parts = [total] + [swapped(total, mask) for mask in masks[1:]]

    solution, objective = pl.pallas_call(
        functools.partial(place_kernel, blocks, height * width),
        in_specs=[smem, anywhere] + [vmem] * len(parts),
        out_specs=[anywhere, smem],
        out_shape=[shape(rows_here, width_here), shape(ITERS)],
        scratch_shapes=[pltpu.SemaphoreType.DMA((blocks,))],
        compiler_params=vmem_grant(1),
        name="place",
    )(senders, arrived, *parts)
    return solution, objective


def solution(mesh):
    placed = (P(ROWS, COLS), P(ROWS, COLS), P(ROWS, COLS), P())
    return jax.shard_map(per_device, mesh=mesh, in_specs=placed, out_specs=(P(ROWS, COLS), P()), check_vma=False)
```

```python
import functools

import jax
import jax.numpy as jnp
from jax import lax
from jax.experimental import pallas as pl
from jax.experimental.pallas import tpu as pltpu
from jax.sharding import PartitionSpec as P

BR = 8
TW = 128
ITERS = 3
HALF = TW // 2
PAD = 16
ROWS, COLS = "rows", "cols"
ALONG_Z = (1, 16, 32)

fidelity_scale = 0.25
tau_step = 0.35
sigma_step = 0.35
tv_weight = 0.3


def vmem_grant(mebibytes):
    return pltpu.CompilerParams(vmem_limit_bytes=int(mebibytes * 2**20))


def tile_fidelity(weight, mask):
    return (tau_step * fidelity_scale * weight.astype(jnp.float32)) * (1 - mask).astype(jnp.float32)


def sides_kernel(tiles, weight, image, mask, swap_a, swap_b, up, down, img, msk, img_rows, msk_rows, sem):
    rows = image.shape[0]
    blocks = rows // BR
    lane = lax.broadcasted_iota(jnp.int32, (BR, TW), 1)
    sub = lax.broadcasted_iota(jnp.int32, (BR, TW), 0)
    copies = []
    for side in range(2):
        column, row = pl.ds(side * (tiles - 1) * TW, TW), pl.ds(side * (rows - BR), BR)
        for source, kept, kept_rows in ((image, img, img_rows), (mask, msk, msk_rows)):
            copies.append(pltpu.make_async_copy(source.at[:, column], kept.at[side], sem.at[len(copies)]))
            copies.append(pltpu.make_async_copy(source.at[row], kept_rows.at[side], sem.at[len(copies)]))
    for copy in copies:
        copy.start()
    for copy in copies:
        copy.wait()
    even = lax.rem(lax.axis_index(COLS), 2) == 0
    for b in range(blocks):
        here = slice(b * BR, (b + 1) * BR)
        f = tile_fidelity(weight[b, 0], msk[0, here])
        to_left = jnp.where(lane < HALF, img[0, here], pltpu.roll(f, HALF, 1))
        f = tile_fidelity(weight[b, tiles - 1], msk[1, here])
        to_right = jnp.where(lane < HALF, pltpu.roll(f, HALF, 1), img[1, here])
        swap_a[here] = jnp.where(even, to_right, to_left)
        swap_b[here] = jnp.where(even, to_left, to_right)
    for t in range(tiles):
        cols = slice(t * TW, (t + 1) * TW)
        f = tile_fidelity(weight[0, t], msk_rows[0, :, cols])
        up[t] = jnp.where(sub < 4, img_rows[0, :, cols], pltpu.roll(f, 4, 0))
        f = tile_fidelity(weight[blocks - 1, t], msk_rows[1, :, cols])
        down[t] = jnp.where(sub < 4, pltpu.roll(img_rows[1, :, cols], 4, 0), f)


def halo_tile(even, side_a, side_b, rows):
    lane = lax.broadcasted_iota(jnp.int32, (BR, TW), 1)
    a, b = side_a[rows], side_b[rows]
    right, left = jnp.where(even, a, b), jnp.where(even, b, a)
    return jnp.where(lane < HALF, right, left), pltpu.roll(jnp.where(lane < HALF, left, right), HALF, 1)


def corners_kernel(tiles, side_a, side_b, up, down, swap_a, swap_b):
    rows = side_a.shape[0]
    sub = lax.broadcasted_iota(jnp.int32, (BR, TW), 0)
    even_col = lax.rem(lax.axis_index(COLS), 2) == 0
    even_row = lax.rem(lax.axis_index(ROWS), 2) == 0

    def put(t, top, bottom):
        swap_a[t] = jnp.where(even_row, bottom, top)
        swap_b[t] = jnp.where(even_row, top, bottom)

    for t in range(tiles):
        put(t, up[t], down[t])
    g, f = halo_tile(even_col, side_a, side_b, slice(0, BR))
    top = jnp.where(sub < 4, g, pltpu.roll(f, 4, 0))
    g, f = halo_tile(even_col, side_a, side_b, slice(rows - BR, rows))
    put(tiles, top, jnp.where(sub < 4, pltpu.roll(g, 4, 0), f))


def solve_kernel(
    tiles, blocks, height, width,
    where_, owner, weight, image, mask, edge_a, edge_b, side_a, side_b,
    slots, partial,
    img, fid, inv, ext, pri, dual_r, dual_c, staged, sem,
):
    rows = blocks * BR
    own_row, own_col = where_[0], where_[1]
    even_row, even_col = lax.rem(own_row, 2) == 0, lax.rem(own_col, 2) == 0
    lane = lax.broadcasted_iota(jnp.int32, (BR, TW), 1)
    sub = lax.broadcasted_iota(jnp.int32, (BR, TW), 0)

    for t in range(tiles):
        for b in range(blocks):
            natural, cols = slice(b * BR, (b + 1) * BR), slice(t * TW, (t + 1) * TW)
            here = slice(PAD + b * BR, PAD + (b + 1) * BR)
            f = tile_fidelity(weight[b, t], mask[natural, cols])
            img[t, here] = image[natural, cols]
            fid[t, here] = f
            inv[t, here] = 1.0 / (1.0 + f)
    low, high = slice(PAD - BR, PAD), slice(PAD + rows, PAD + rows + BR)
    for t in range(tiles + 1):
        a, b = edge_a[t], edge_b[t]
        v, w = jnp.where(even_row, b, a), jnp.where(even_row, a, b)
        for at, g, f in (
            (low, jnp.where(sub >= 4, pltpu.roll(v, 4, 0), 0.0), jnp.where(sub >= 4, v, 0.0)),
            (high, jnp.where(sub < 4, w, 0.0), jnp.where(sub < 4, pltpu.roll(w, 4, 0), 0.0)),
        ):
            img[t, at] = g
            fid[t, at] = f
            inv[t, at] = 1.0 / (1.0 + f)
    for b in range(blocks):
        here = slice(PAD + b * BR, PAD + (b + 1) * BR)
        g, f = halo_tile(even_col, side_a, side_b, slice(b * BR, (b + 1) * BR))
        img[tiles, here] = g
        fid[tiles, here] = f
        inv[tiles, here] = 1.0 / (1.0 + f)

    col = own_col * (tiles * TW) + lane
    inner_last = col + (tiles - 1) * TW < width - 1
    halo_col = jnp.where(lane < HALF, col + tiles * TW, col - TW)
    inner_halo = (halo_col >= 0) & (halo_col < width - 1)

    def send(b):
        return pltpu.make_async_copy(staged.at[b], slots.at[owner[own_row * blocks + b]], sem.at[b])

    def sweep(k, start, acc, only_duals=False):
        base = PAD + start
        here, lower, upper = pl.ds(base, BR), pl.ds(base + 1, BR), pl.ds(base - 1, BR)
        first, final = k == 0, k == ITERS - 1
        source = img if first else ext
        row = own_row * rows + start + sub
        inner_row = (row >= 0) & (row < height - 1)

        def duals(t, e, right):
            g_r = source[t, lower] - e
            if start < 0 or start + BR >= rows:
                g_r = jnp.where(inner_row, g_r, 0.0)
            g_c = right - e
            if t == tiles - 1:
                g_c = jnp.where(inner_last, g_c, 0.0)
            if t == tiles:
                g_c = jnp.where(inner_halo, g_c, 0.0)
            n = g_r * g_r + g_c * g_c
            s = lax.rsqrt(n)
            steep = jnp.where(n > 0.0, n * s, 0.0)
            q_r, q_c = g_r, g_c
            if not first:
                q_r, q_c = dual_r[t, here] + q_r, dual_c[t, here] + q_c
                s = lax.rsqrt(q_r * q_r + q_c * q_c)
            scale = jnp.minimum(1.0, (tv_weight / sigma_step) * s)
            d_r, d_c = q_r * scale, q_c * scale
            dual_r[t, here] = d_r
            if not final:
                dual_c[t, here] = d_c
            return steep, d_r, d_c

        def update(t, e, d_r, d_c, left, pull):
            div = d_r - dual_r[t, upper] + (d_c - left)
            p = e if first else pri[t, here]
            u = (p + (tau_step * sigma_step) * div + pull) * inv[t, here]
            if final:
                staged[start // BR, :, t * TW:(t + 1) * TW] = u
            else:
                ext[t, here] = u + (u - p)
                pri[t, here] = u
            return u

        e_halo = source[tiles, here]
        e = source[0, here]
        turned = pltpu.roll(e, TW - 1, 1)
        turned_halo = pltpu.roll(e_halo, TW - 1, 1)
        _, h_r, h_c = duals(tiles, e_halo, jnp.where(lane == TW - 1, turned, turned_halo))
        shifted = pltpu.roll(h_c, 1, 1)
        shifted_halo = shifted
        fit, tv = acc
        for t in range(tiles):
            if t < tiles - 1:
                e_next = source[t + 1, here]
                turned_next = pltpu.roll(e_next, TW - 1, 1)
            else:
                e_next, turned_next = None, turned_halo
            steep, d_r, d_c = duals(t, e, jnp.where(lane == TW - 1, turned_next, turned))
            if only_duals:
                e, turned = e_next, turned_next
                continue
            shifted_here = pltpu.roll(d_c, 1, 1)
            g, f = img[t, here], fid[t, here]
            u = update(t, e, d_r, d_c, jnp.where(lane == 0, shifted, shifted_here), f * g)
            miss = u - g
            loss = f * (miss * miss)
            if start < 0:
                loss, steep = jnp.where(sub >= -start, loss, 0.0), jnp.where(sub >= -start, steep, 0.0)
            elif start + BR > rows:
                loss, steep = jnp.where(sub < rows - start, loss, 0.0), jnp.where(sub < rows - start, steep, 0.0)
            fit, tv = fit + loss, tv + steep
            shifted, e, turned = shifted_here, e_next, turned_next
        if not final:
            update(tiles, e_halo, h_r, h_c, jnp.where(lane == 0, shifted, shifted_halo), fid[tiles, here] * img[tiles, here])
        return fit, tv

    zero = jnp.zeros((BR, TW), jnp.float32)
    total = zero
    for k in range(ITERS):
        acc = zero, zero
        if k < ITERS - 1:
            for start in range(-BR // 2, rows, BR):
                acc = sweep(k, start, acc)
        else:
            sweep(k, -BR, acc, only_duals=True)
            for b in range(blocks):
                acc = sweep(k, b * BR, acc)
                if b:
                    send(b - 1).start()
        fit, tv = acc
        total = jnp.where(lane == k, jnp.sum((0.5 / tau_step) * fit + tv_weight * tv), total)
    send(blocks - 1).start()
    partial[...] = total
    for b in range(blocks):
        send(b).wait()


def lookup_kernel(blocks, where_, owner, senders):
    def body(sender, found):
        mine = owner[sender * blocks] == where_[0]
        for i in range(1, blocks):
            mine |= owner[sender * blocks + i] == where_[0]
        senders[found] = sender
        return found + mine.astype(jnp.int32)

    lax.fori_loop(0, owner.shape[0] // blocks, body, jnp.int32(0))


def place_kernel(blocks, pixels, senders, arrived, *refs):
    parts, (out, objective, sums, sem) = refs[:-4], refs[-4:]
    copies = [
        pltpu.make_async_copy(arrived.at[senders[k]], out.at[pl.ds(k * BR, BR)], sem.at[k]) for k in range(blocks)
    ]
    for copy in copies:
        copy.start()
    values = [part[...] for part in parts]
    while len(values) > 1:
        values = [a + b for a, b in zip(values[::2], values[1::2])]
    lane = lax.broadcasted_iota(jnp.int32, values[0].shape, 1)
    for k in range(ITERS):
        sums[k] = jnp.sum(jnp.where(lane == k, values[0], 0.0)) / pixels
    copies.append(pltpu.make_async_copy(sums, objective, sem.at[blocks]))
    copies[-1].start()
    for copy in copies:
        copy.wait()


def per_device(image, cloud_mask, tile_weight, owner):
    rows_here, width_here = image.shape
    blocks, tiles = rows_here // BR, width_here // TW
    row_count, col_count = lax.axis_size(ROWS), lax.axis_size(COLS)
    height, width = rows_here * row_count, width_here * col_count
    own_row, own_col = lax.axis_index(ROWS), lax.axis_index(COLS)
    where_ = jnp.stack([own_row, own_col]).astype(jnp.int32)
    smem, vmem, hbm, anywhere = (pl.BlockSpec(memory_space=s) for s in (pltpu.SMEM, pltpu.VMEM, pltpu.HBM, pl.ANY))

    def shape(*dims):
        return jax.ShapeDtypeStruct(dims, jnp.float32)

    def work(flops):
        return pl.CostEstimate(flops=flops, bytes_accessed=0, transcendentals=0)

    def swap(array, axis, first):
        pairs = [(i, i + 1) for i in range(first, lax.axis_size(axis) - 1, 2)]
        return lax.ppermute(array, axis, pairs + [(j, i) for i, j in pairs])

    edge = shape(tiles + 1, BR, TW)
    side_a, side_b, up, down = pl.pallas_call(
        functools.partial(sides_kernel, tiles),
        in_specs=[smem, hbm, hbm],
        out_specs=[vmem] * 4,
        out_shape=[shape(rows_here, TW)] * 2 + [edge] * 2,
        scratch_shapes=[
            pltpu.VMEM((2, rows_here, TW), jnp.float32),
            pltpu.VMEM((2, rows_here, TW), jnp.int32),
            pltpu.VMEM((2, BR, width_here), jnp.float32),
            pltpu.VMEM((2, BR, width_here), jnp.int32),
            pltpu.SemaphoreType.DMA((8,)),
        ],
        cost_estimate=work(2 * 10**9),
        compiler_params=vmem_grant(53.5),
        name="sides",
    )(tile_weight, image, cloud_mask)
    side_a, side_b = swap(side_a, COLS, 0), swap(side_b, COLS, 1)
    edge_a, edge_b = pl.pallas_call(
        functools.partial(corners_kernel, tiles),
        in_specs=[vmem] * 4,
        out_specs=[vmem] * 2,
        out_shape=[edge] * 2,
        cost_estimate=work(2 * 10**9),
        compiler_params=vmem_grant(2),
        name="corners",
    )(side_a, side_b, up, down)
    edge_a, edge_b = swap(edge_a, ROWS, 0), swap(edge_b, ROWS, 1)
    slots, partial = pl.pallas_call(
        functools.partial(solve_kernel, tiles, blocks, height, width),
        in_specs=[smem] * 3 + [vmem] * 6,
        out_specs=[hbm, vmem],
        out_shape=[shape(row_count, BR, width_here), shape(BR, TW)],
        scratch_shapes=[pltpu.VMEM((tiles + 1, PAD + rows_here + PAD, TW), jnp.float32)] * 7
        + [pltpu.VMEM((blocks, BR, width_here), jnp.float32), pltpu.SemaphoreType.DMA((blocks,))],
        compiler_params=vmem_grant(52),
        name="solve",
    )(where_, owner, tile_weight, image, cloud_mask, edge_a, edge_b, side_a, side_b)
    arrived = lax.all_to_all(slots, ROWS, split_axis=0, concat_axis=0, tiled=True)

    later, _ = lax.optimization_barrier((owner, partial))
    senders = pl.pallas_call(
        functools.partial(lookup_kernel, blocks),
        in_specs=[smem, smem],
        out_specs=smem,
        out_shape=jax.ShapeDtypeStruct((2 * blocks,), jnp.int32),
        compiler_params=vmem_grant(1),
        name="lookup",
    )(where_, later)

    devices = row_count * col_count

    def swapped(array, mask):
        return lax.ppermute(array, (ROWS, COLS), [(i, i ^ mask) for i in range(devices)])

    total = partial[:1]
    for bit in (1 << i for i in range(devices.bit_length() - 1)):
        if bit not in ALONG_Z:
            total = total + swapped(total, bit)
    masks = [0]
    for bit in ALONG_Z:
        masks += [mask | bit for mask in masks]
    parts = [total] + [swapped(total, mask) for mask in masks[1:]]

    solution, objective = pl.pallas_call(
        functools.partial(place_kernel, blocks, height * width),
        in_specs=[smem, anywhere] + [vmem] * len(parts),
        out_specs=[anywhere, anywhere],
        out_shape=[shape(rows_here, width_here), shape(ITERS)],
        scratch_shapes=[pltpu.SMEM((ITERS,), jnp.float32), pltpu.SemaphoreType.DMA((blocks + 1,))],
        compiler_params=vmem_grant(1),
        name="place",
    )(senders, arrived, *parts)
    return solution, objective


def solution(mesh):
    placed = (P(ROWS, COLS), P(ROWS, COLS), P(ROWS, COLS), P())
    return jax.shard_map(per_device, mesh=mesh, in_specs=placed, out_specs=(P(ROWS, COLS), P()), check_vma=False)
```

```python
import functools

import jax
import jax.numpy as jnp
from jax import lax
from jax.experimental import pallas as pl
from jax.experimental.pallas import tpu as pltpu
from jax.sharding import PartitionSpec as P

BR = 8
TW = 128
ITERS = 3
HALF = TW // 2
SIDE = 8
PAD = 16
ROWS, COLS = "rows", "cols"
ALONG_Z = (1, 16, 32)

fidelity_scale = 0.25
tau_step = 0.35
sigma_step = 0.35
tv_weight = 0.3


def vmem_grant(mebibytes):
    return pltpu.CompilerParams(vmem_limit_bytes=int(mebibytes * 2**20))


def tile_fidelity(weight, mask):
    return (tau_step * fidelity_scale * weight.astype(jnp.float32)) * (1 - mask).astype(jnp.float32)


def turned(tile, shift):
    return pltpu.roll(tile, shift % TW, 1) if shift % TW else tile


def sides_kernel(tiles, weight, image, mask, swap_a, swap_b, up, down, img, msk, img_rows, msk_rows, sem):
    rows = image.shape[0]
    blocks = rows // BR
    lane = lax.broadcasted_iota(jnp.int32, (BR, TW), 1)
    sub = lax.broadcasted_iota(jnp.int32, (BR, TW), 0)
    copies = []
    for side in range(2):
        column, row = pl.ds(side * (tiles - 1) * TW, TW), pl.ds(side * (rows - BR), BR)
        for source, kept, kept_rows in ((image, img, img_rows), (mask, msk, msk_rows)):
            copies.append(pltpu.make_async_copy(source.at[:, column], kept.at[side], sem.at[len(copies)]))
            copies.append(pltpu.make_async_copy(source.at[row], kept_rows.at[side], sem.at[len(copies)]))
    for copy in copies:
        copy.start()
    for copy in copies:
        copy.wait()
    to_left = to_right = jnp.zeros((BR, TW), jnp.float32)
    for b in range(blocks):
        here = slice(b * BR, (b + 1) * BR)
        at = b * 2 * SIDE
        for shift, value in ((at, img[0, here]), (at + SIDE, tile_fidelity(weight[b, 0], msk[0, here]))):
            to_left = jnp.where((lane >= shift) & (lane < shift + SIDE), turned(value, shift), to_left)
        for shift, value in ((at, img[1, here]), (at + SIDE, tile_fidelity(weight[b, tiles - 1], msk[1, here]))):
            to_right = jnp.where((lane >= shift) & (lane < shift + SIDE), turned(value, shift + SIDE), to_right)
    even = lax.rem(lax.axis_index(COLS), 2) == 0
    swap_a[...] = jnp.where(even, to_right, to_left)
    swap_b[...] = jnp.where(even, to_left, to_right)
    for t in range(tiles):
        cols = slice(t * TW, (t + 1) * TW)
        f = tile_fidelity(weight[0, t], msk_rows[0, :, cols])
        up[t] = jnp.where(sub < 4, img_rows[0, :, cols], pltpu.roll(f, 4, 0))
        f = tile_fidelity(weight[blocks - 1, t], msk_rows[1, :, cols])
        down[t] = jnp.where(sub < 4, pltpu.roll(img_rows[1, :, cols], 4, 0), f)


def halo_tile(even, side_a, side_b, block):
    lane = lax.broadcasted_iota(jnp.int32, (BR, TW), 1)
    a, b = side_a[...], side_b[...]
    right, left = jnp.where(even, a, b), jnp.where(even, b, a)
    at = block * 2 * SIDE

    def spread(at):
        return jnp.where(lane < HALF, turned(right, -at), turned(left, -at - SIDE))

    return spread(at), spread(at + SIDE)


def corners_kernel(tiles, blocks, side_a, side_b, up, down, swap_a, swap_b):
    sub = lax.broadcasted_iota(jnp.int32, (BR, TW), 0)
    even_col = lax.rem(lax.axis_index(COLS), 2) == 0
    even_row = lax.rem(lax.axis_index(ROWS), 2) == 0

    def put(t, top, bottom):
        swap_a[t] = jnp.where(even_row, bottom, top)
        swap_b[t] = jnp.where(even_row, top, bottom)

    for t in range(tiles):
        put(t, up[t], down[t])
    g, f = halo_tile(even_col, side_a, side_b, 0)
    top = jnp.where(sub < 4, g, pltpu.roll(f, 4, 0))
    g, f = halo_tile(even_col, side_a, side_b, blocks - 1)
    put(tiles, top, jnp.where(sub < 4, pltpu.roll(g, 4, 0), f))


def solve_kernel(
    tiles, blocks, height, width,
    where_, owner, weight, image, mask, edge_a, edge_b, side_a, side_b,
    slots, partial,
    img, fid, inv, ext, pri, dual_r, dual_c, staged, sem,
):
    rows = blocks * BR
    own_row, own_col = where_[0], where_[1]
    even_row, even_col = lax.rem(own_row, 2) == 0, lax.rem(own_col, 2) == 0
    lane = lax.broadcasted_iota(jnp.int32, (BR, TW), 1)
    sub = lax.broadcasted_iota(jnp.int32, (BR, TW), 0)

    for t in range(tiles):
        for b in range(blocks):
            natural, cols = slice(b * BR, (b + 1) * BR), slice(t * TW, (t + 1) * TW)
            here = slice(PAD + b * BR, PAD + (b + 1) * BR)
            f = tile_fidelity(weight[b, t], mask[natural, cols])
            img[t, here] = image[natural, cols]
            fid[t, here] = f
            inv[t, here] = 1.0 / (1.0 + f)
    low, high = slice(PAD - BR, PAD), slice(PAD + rows, PAD + rows + BR)
    for t in range(tiles + 1):
        a, b = edge_a[t], edge_b[t]
        v, w = jnp.where(even_row, b, a), jnp.where(even_row, a, b)
        for at, g, f in (
            (low, jnp.where(sub >= 4, pltpu.roll(v, 4, 0), 0.0), jnp.where(sub >= 4, v, 0.0)),
            (high, jnp.where(sub < 4, w, 0.0), jnp.where(sub < 4, pltpu.roll(w, 4, 0), 0.0)),
        ):
            img[t, at] = g
            fid[t, at] = f
            inv[t, at] = 1.0 / (1.0 + f)
    for b in range(blocks):
        here = slice(PAD + b * BR, PAD + (b + 1) * BR)
        g, f = halo_tile(even_col, side_a, side_b, b)
        img[tiles, here] = g
        fid[tiles, here] = f
        inv[tiles, here] = 1.0 / (1.0 + f)

    col = own_col * (tiles * TW) + lane
    inner_last = col + (tiles - 1) * TW < width - 1
    halo_col = jnp.where(lane < HALF, col + tiles * TW, col - TW)
    inner_halo = (halo_col >= 0) & (halo_col < width - 1)

    def send(b):
        return pltpu.make_async_copy(staged.at[b], slots.at[owner[own_row * blocks + b]], sem.at[b])

    def sweep(k, start, acc, only_duals=False):
        base = PAD + start
        here, lower, upper = pl.ds(base, BR), pl.ds(base + 1, BR), pl.ds(base - 1, BR)
        first, final = k == 0, k == ITERS - 1
        source = img if first else ext
        row = own_row * rows + start + sub
        inner_row = (row >= 0) & (row < height - 1)

        def duals(t, e, right):
            g_r = source[t, lower] - e
            if start < 0 or start + BR >= rows:
                g_r = jnp.where(inner_row, g_r, 0.0)
            g_c = right - e
            if t == tiles - 1:
                g_c = jnp.where(inner_last, g_c, 0.0)
            if t == tiles:
                g_c = jnp.where(inner_halo, g_c, 0.0)
            n = g_r * g_r + g_c * g_c
            s = lax.rsqrt(n)
            steep = jnp.where(n > 0.0, n * s, 0.0)
            q_r, q_c = g_r, g_c
            if not first:
                q_r, q_c = dual_r[t, here] + q_r, dual_c[t, here] + q_c
                s = lax.rsqrt(q_r * q_r + q_c * q_c)
            scale = jnp.minimum(1.0, (tv_weight / sigma_step) * s)
            d_r, d_c = q_r * scale, q_c * scale
            dual_r[t, here] = d_r
            if not final:
                dual_c[t, here] = d_c
            return steep, d_r, d_c

        def update(t, e, d_r, d_c, left, pull):
            div = d_r - dual_r[t, upper] + (d_c - left)
            p = e if first else pri[t, here]
            u = (p + (tau_step * sigma_step) * div + pull) * inv[t, here]
            if final:
                staged[start // BR, :, t * TW:(t + 1) * TW] = u
            else:
                ext[t, here] = u + (u - p)
                pri[t, here] = u
            return u

        e_halo = source[tiles, here]
        e = source[0, here]
        turned = pltpu.roll(e, TW - 1, 1)
        turned_halo = pltpu.roll(e_halo, TW - 1, 1)
        _, h_r, h_c = duals(tiles, e_halo, jnp.where(lane == TW - 1, turned, turned_halo))
        shifted = pltpu.roll(h_c, 1, 1)
        shifted_halo = shifted
        fit, tv = acc
        for t in range(tiles):
            if t < tiles - 1:
                e_next = source[t + 1, here]
                turned_next = pltpu.roll(e_next, TW - 1, 1)
            else:
                e_next, turned_next = None, turned_halo
            steep, d_r, d_c = duals(t, e, jnp.where(lane == TW - 1, turned_next, turned))
            if only_duals:
                e, turned = e_next, turned_next
                continue
            shifted_here = pltpu.roll(d_c, 1, 1)
            g, f = img[t, here], fid[t, here]
            u = update(t, e, d_r, d_c, jnp.where(lane == 0, shifted, shifted_here), f * g)
            miss = u - g
            loss = f * (miss * miss)
            if start < 0:
                loss, steep = jnp.where(sub >= -start, loss, 0.0), jnp.where(sub >= -start, steep, 0.0)
            elif start + BR > rows:
                loss, steep = jnp.where(sub < rows - start, loss, 0.0), jnp.where(sub < rows - start, steep, 0.0)
            fit, tv = fit + loss, tv + steep
            shifted, e, turned = shifted_here, e_next, turned_next
        if not final:
            update(tiles, e_halo, h_r, h_c, jnp.where(lane == 0, shifted, shifted_halo), fid[tiles, here] * img[tiles, here])
        return fit, tv

    zero = jnp.zeros((BR, TW), jnp.float32)
    total = zero
    for k in range(ITERS):
        acc = zero, zero
        if k < ITERS - 1:
            for start in range(-BR // 2, rows, BR):
                acc = sweep(k, start, acc)
        else:
            sweep(k, -BR, acc, only_duals=True)
            for b in range(blocks):
                acc = sweep(k, b * BR, acc)
                if b:
                    send(b - 1).start()
        fit, tv = acc
        total = jnp.where(lane == k, jnp.sum((0.5 / tau_step) * fit + tv_weight * tv), total)
    send(blocks - 1).start()
    partial[...] = total
    for b in range(blocks):
        send(b).wait()


def lookup_kernel(blocks, where_, owner, senders):
    def body(sender, found):
        mine = owner[sender * blocks] == where_[0]
        for i in range(1, blocks):
            mine |= owner[sender * blocks + i] == where_[0]
        senders[found] = sender
        return found + mine.astype(jnp.int32)

    lax.fori_loop(0, owner.shape[0] // blocks, body, jnp.int32(0))


def place_kernel(blocks, pixels, senders, arrived, *refs):
    parts, (out, objective, sums, sem) = refs[:-4], refs[-4:]
    copies = [
        pltpu.make_async_copy(arrived.at[senders[k]], out.at[pl.ds(k * BR, BR)], sem.at[k]) for k in range(blocks)
    ]
    for copy in copies:
        copy.start()
    values = [part[...] for part in parts]
    while len(values) > 1:
        values = [a + b for a, b in zip(values[::2], values[1::2])]
    lane = lax.broadcasted_iota(jnp.int32, values[0].shape, 1)
    for k in range(ITERS):
        sums[k] = jnp.sum(jnp.where(lane == k, values[0], 0.0)) / pixels
    copies.append(pltpu.make_async_copy(sums, objective, sem.at[blocks]))
    copies[-1].start()
    for copy in copies:
        copy.wait()


def per_device(image, cloud_mask, tile_weight, owner):
    rows_here, width_here = image.shape
    blocks, tiles = rows_here // BR, width_here // TW
    row_count, col_count = lax.axis_size(ROWS), lax.axis_size(COLS)
    height, width = rows_here * row_count, width_here * col_count
    own_row, own_col = lax.axis_index(ROWS), lax.axis_index(COLS)
    where_ = jnp.stack([own_row, own_col]).astype(jnp.int32)
    smem, vmem, hbm, anywhere = (pl.BlockSpec(memory_space=s) for s in (pltpu.SMEM, pltpu.VMEM, pltpu.HBM, pl.ANY))

    def shape(*dims):
        return jax.ShapeDtypeStruct(dims, jnp.float32)

    def work(flops):
        return pl.CostEstimate(flops=flops, bytes_accessed=0, transcendentals=0)

    def swap(array, axis, first):
        pairs = [(i, i + 1) for i in range(first, lax.axis_size(axis) - 1, 2)]
        return lax.ppermute(array, axis, pairs + [(j, i) for i, j in pairs])

    edge = shape(tiles + 1, BR, TW)
    side_a, side_b, up, down = pl.pallas_call(
        functools.partial(sides_kernel, tiles),
        in_specs=[smem, hbm, hbm],
        out_specs=[vmem] * 4,
        out_shape=[shape(BR, TW)] * 2 + [edge] * 2,
        scratch_shapes=[
            pltpu.VMEM((2, rows_here, TW), jnp.float32),
            pltpu.VMEM((2, rows_here, TW), jnp.int32),
            pltpu.VMEM((2, BR, width_here), jnp.float32),
            pltpu.VMEM((2, BR, width_here), jnp.int32),
            pltpu.SemaphoreType.DMA((8,)),
        ],
        cost_estimate=work(2 * 10**9),
        compiler_params=vmem_grant(53.5),
        name="sides",
    )(tile_weight, image, cloud_mask)
    side_a, side_b = swap(side_a, COLS, 0), swap(side_b, COLS, 1)
    edge_a, edge_b = pl.pallas_call(
        functools.partial(corners_kernel, tiles, blocks),
        in_specs=[vmem] * 4,
        out_specs=[vmem] * 2,
        out_shape=[edge] * 2,
        cost_estimate=work(2 * 10**9),
        compiler_params=vmem_grant(2),
        name="corners",
    )(side_a, side_b, up, down)
    edge_a, edge_b = swap(edge_a, ROWS, 0), swap(edge_b, ROWS, 1)
    slots, partial = pl.pallas_call(
        functools.partial(solve_kernel, tiles, blocks, height, width),
        in_specs=[smem] * 3 + [vmem] * 6,
        out_specs=[hbm, vmem],
        out_shape=[shape(row_count, BR, width_here), shape(BR, TW)],
        scratch_shapes=[pltpu.VMEM((tiles + 1, PAD + rows_here + PAD, TW), jnp.float32)] * 7
        + [pltpu.VMEM((blocks, BR, width_here), jnp.float32), pltpu.SemaphoreType.DMA((blocks,))],
        compiler_params=vmem_grant(52),
        name="solve",
    )(where_, owner, tile_weight, image, cloud_mask, edge_a, edge_b, side_a, side_b)
    arrived = lax.all_to_all(slots, ROWS, split_axis=0, concat_axis=0, tiled=True)

    later, _ = lax.optimization_barrier((owner, partial))
    senders = pl.pallas_call(
        functools.partial(lookup_kernel, blocks),
        in_specs=[smem, smem],
        out_specs=smem,
        out_shape=jax.ShapeDtypeStruct((2 * blocks,), jnp.int32),
        compiler_params=vmem_grant(1),
        name="lookup",
    )(where_, later)

    devices = row_count * col_count

    def swapped(array, mask):
        return lax.ppermute(array, (ROWS, COLS), [(i, i ^ mask) for i in range(devices)])

    total = partial[:1]
    for bit in (1 << i for i in range(devices.bit_length() - 1)):
        if bit not in ALONG_Z:
            total = total + swapped(total, bit)
    masks = [0]
    for bit in ALONG_Z:
        masks += [mask | bit for mask in masks]
    parts = [total] + [swapped(total, mask) for mask in masks[1:]]

    solution, objective = pl.pallas_call(
        functools.partial(place_kernel, blocks, height * width),
        in_specs=[smem, anywhere] + [vmem] * len(parts),
        out_specs=[anywhere, anywhere],
        out_shape=[shape(rows_here, width_here), shape(ITERS)],
        scratch_shapes=[pltpu.SMEM((ITERS,), jnp.float32), pltpu.SemaphoreType.DMA((blocks + 1,))],
        compiler_params=vmem_grant(1),
        name="place",
    )(senders, arrived, *parts)
    return solution, objective


def solution(mesh):
    placed = (P(ROWS, COLS), P(ROWS, COLS), P(ROWS, COLS), P())
    return jax.shard_map(per_device, mesh=mesh, in_specs=placed, out_specs=(P(ROWS, COLS), P()), check_vma=False)
```

```python
import functools

import jax
import jax.numpy as jnp
from jax import lax
from jax.experimental import pallas as pl
from jax.experimental.pallas import tpu as pltpu
from jax.sharding import PartitionSpec as P

BR = 8
TW = 128
ITERS = 3
HALF = TW // 2
SIDE = 8
PAD = 16
ROWS, COLS = "rows", "cols"
ALONG_Z = (1, 16, 32)

fidelity_scale = 0.25
tau_step = 0.35
sigma_step = 0.35
tv_weight = 0.3


def vmem_grant(mebibytes):
    return pltpu.CompilerParams(vmem_limit_bytes=int(mebibytes * 2**20))


def tile_fidelity(weight, mask):
    return (tau_step * fidelity_scale * weight.astype(jnp.float32)) * (1 - mask).astype(jnp.float32)


def turned(tile, shift):
    return pltpu.roll(tile, shift % TW, 1) if shift % TW else tile


def sides_kernel(tiles, weight, image, mask, swap_a, swap_b, up, down, img, msk, img_rows, msk_rows, sem):
    rows = image.shape[0]
    blocks = rows // BR
    lane = lax.broadcasted_iota(jnp.int32, (BR, TW), 1)
    sub = lax.broadcasted_iota(jnp.int32, (BR, TW), 0)
    copies = []
    for side in range(2):
        column, row = pl.ds(side * (tiles - 1) * TW, TW), pl.ds(side * (rows - BR), BR)
        for source, kept, kept_rows in ((image, img, img_rows), (mask, msk, msk_rows)):
            copies.append(pltpu.make_async_copy(source.at[:, column], kept.at[side], sem.at[len(copies)]))
            copies.append(pltpu.make_async_copy(source.at[row], kept_rows.at[side], sem.at[len(copies)]))
    for copy in copies:
        copy.start()
    for copy in copies:
        copy.wait()
    to_left = to_right = jnp.zeros((BR, TW), jnp.float32)
    for b in range(blocks):
        here = slice(b * BR, (b + 1) * BR)
        at = b * 2 * SIDE
        for shift, value in ((at, img[0, here]), (at + SIDE, tile_fidelity(weight[b, 0], msk[0, here]))):
            to_left = jnp.where((lane >= shift) & (lane < shift + SIDE), turned(value, shift), to_left)
        for shift, value in ((at, img[1, here]), (at + SIDE, tile_fidelity(weight[b, tiles - 1], msk[1, here]))):
            to_right = jnp.where((lane >= shift) & (lane < shift + SIDE), turned(value, shift + SIDE), to_right)
    even = lax.rem(lax.axis_index(COLS), 2) == 0
    swap_a[...] = jnp.where(even, to_right, to_left)
    swap_b[...] = jnp.where(even, to_left, to_right)
    for t in range(tiles):
        cols = slice(t * TW, (t + 1) * TW)
        f = tile_fidelity(weight[0, t], msk_rows[0, :, cols])
        up[t] = jnp.where(sub < 4, img_rows[0, :, cols], pltpu.roll(f, 4, 0))
        f = tile_fidelity(weight[blocks - 1, t], msk_rows[1, :, cols])
        down[t] = jnp.where(sub < 4, pltpu.roll(img_rows[1, :, cols], 4, 0), f)


def halo_tile(even, side_a, side_b, block):
    lane = lax.broadcasted_iota(jnp.int32, (BR, TW), 1)
    a, b = side_a[...], side_b[...]
    right, left = jnp.where(even, a, b), jnp.where(even, b, a)
    at = block * 2 * SIDE

    def spread(at):
        return jnp.where(lane < HALF, turned(right, -at), turned(left, -at - SIDE))

    return spread(at), spread(at + SIDE)


def corners_kernel(tiles, blocks, side_a, side_b, up, down, swap_b, swap_a):
    sub = lax.broadcasted_iota(jnp.int32, (BR, TW), 0)
    even_col = lax.rem(lax.axis_index(COLS), 2) == 0
    even_row = lax.rem(lax.axis_index(ROWS), 2) == 0

    def put(t, top, bottom):
        swap_a[t] = jnp.where(even_row, bottom, top)
        swap_b[t] = jnp.where(even_row, top, bottom)

    for t in range(tiles):
        put(t, up[t], down[t])
    g, f = halo_tile(even_col, side_a, side_b, 0)
    top = jnp.where(sub < 4, g, pltpu.roll(f, 4, 0))
    g, f = halo_tile(even_col, side_a, side_b, blocks - 1)
    put(tiles, top, jnp.where(sub < 4, pltpu.roll(g, 4, 0), f))


def solve_kernel(
    tiles, blocks, height, width,
    where_, owner, weight, image, mask, edge_b, edge_a, side_a, side_b,
    slots, partial,
    img, fid, inv, ext, pri, dual_r, dual_c, staged, sem,
):
    rows = blocks * BR
    own_row, own_col = where_[0], where_[1]
    even_row, even_col = lax.rem(own_row, 2) == 0, lax.rem(own_col, 2) == 0
    lane = lax.broadcasted_iota(jnp.int32, (BR, TW), 1)
    sub = lax.broadcasted_iota(jnp.int32, (BR, TW), 0)

    for t in range(tiles):
        for b in range(blocks):
            natural, cols = slice(b * BR, (b + 1) * BR), slice(t * TW, (t + 1) * TW)
            here = slice(PAD + b * BR, PAD + (b + 1) * BR)
            f = tile_fidelity(weight[b, t], mask[natural, cols])
            img[t, here] = image[natural, cols]
            fid[t, here] = f
            inv[t, here] = 1.0 / (1.0 + f)
    low, high = slice(PAD - BR, PAD), slice(PAD + rows, PAD + rows + BR)
    for t in range(tiles + 1):
        a, b = edge_a[t], edge_b[t]
        v, w = jnp.where(even_row, b, a), jnp.where(even_row, a, b)
        for at, g, f in (
            (low, jnp.where(sub >= 4, pltpu.roll(v, 4, 0), 0.0), jnp.where(sub >= 4, v, 0.0)),
            (high, jnp.where(sub < 4, w, 0.0), jnp.where(sub < 4, pltpu.roll(w, 4, 0), 0.0)),
        ):
            img[t, at] = g
            fid[t, at] = f
            inv[t, at] = 1.0 / (1.0 + f)
    for b in range(blocks):
        here = slice(PAD + b * BR, PAD + (b + 1) * BR)
        g, f = halo_tile(even_col, side_a, side_b, b)
        img[tiles, here] = g
        fid[tiles, here] = f
        inv[tiles, here] = 1.0 / (1.0 + f)

    col = own_col * (tiles * TW) + lane
    inner_last = col + (tiles - 1) * TW < width - 1
    halo_col = jnp.where(lane < HALF, col + tiles * TW, col - TW)
    inner_halo = (halo_col >= 0) & (halo_col < width - 1)

    def send(b):
        return pltpu.make_async_copy(staged.at[b], slots.at[owner[own_row * blocks + b]], sem.at[b])

    def sweep(k, start, acc, only_duals=False):
        base = PAD + start
        here, lower, upper = pl.ds(base, BR), pl.ds(base + 1, BR), pl.ds(base - 1, BR)
        first, final = k == 0, k == ITERS - 1
        source = img if first else ext
        row = own_row * rows + start + sub
        inner_row = (row >= 0) & (row < height - 1)

        def duals(t, e, right):
            g_r = source[t, lower] - e
            if start < 0 or start + BR >= rows:
                g_r = jnp.where(inner_row, g_r, 0.0)
            g_c = right - e
            if t == tiles - 1:
                g_c = jnp.where(inner_last, g_c, 0.0)
            if t == tiles:
                g_c = jnp.where(inner_halo, g_c, 0.0)
            n = g_r * g_r + g_c * g_c
            s = lax.rsqrt(n)
            steep = jnp.where(n > 0.0, n * s, 0.0)
            q_r, q_c = g_r, g_c
            if not first:
                q_r, q_c = dual_r[t, here] + q_r, dual_c[t, here] + q_c
                s = lax.rsqrt(q_r * q_r + q_c * q_c)
            scale = jnp.minimum(1.0, (tv_weight / sigma_step) * s)
            d_r, d_c = q_r * scale, q_c * scale
            dual_r[t, here] = d_r
            if not final:
                dual_c[t, here] = d_c
            return steep, d_r, d_c

        def update(t, e, d_r, d_c, left, pull):
            div = d_r - dual_r[t, upper] + (d_c - left)
            p = e if first else pri[t, here]
            u = (p + (tau_step * sigma_step) * div + pull) * inv[t, here]
            if final:
                staged[start // BR, :, t * TW:(t + 1) * TW] = u
            else:
                ext[t, here] = u + (u - p)
                pri[t, here] = u
            return u

        e_halo = source[tiles, here]
        e = source[0, here]
        turned = pltpu.roll(e, TW - 1, 1)
        turned_halo = pltpu.roll(e_halo, TW - 1, 1)
        _, h_r, h_c = duals(tiles, e_halo, jnp.where(lane == TW - 1, turned, turned_halo))
        shifted = pltpu.roll(h_c, 1, 1)
        shifted_halo = shifted
        fit, tv = acc
        for t in range(tiles):
            if t < tiles - 1:
                e_next = source[t + 1, here]
                turned_next = pltpu.roll(e_next, TW - 1, 1)
            else:
                e_next, turned_next = None, turned_halo
            steep, d_r, d_c = duals(t, e, jnp.where(lane == TW - 1, turned_next, turned))
            if only_duals:
                e, turned = e_next, turned_next
                continue
            shifted_here = pltpu.roll(d_c, 1, 1)
            g, f = img[t, here], fid[t, here]
            u = update(t, e, d_r, d_c, jnp.where(lane == 0, shifted, shifted_here), f * g)
            miss = u - g
            loss = f * (miss * miss)
            if start < 0:
                loss, steep = jnp.where(sub >= -start, loss, 0.0), jnp.where(sub >= -start, steep, 0.0)
            elif start + BR > rows:
                loss, steep = jnp.where(sub < rows - start, loss, 0.0), jnp.where(sub < rows - start, steep, 0.0)
            fit, tv = fit + loss, tv + steep
            shifted, e, turned = shifted_here, e_next, turned_next
        if not final:
            update(tiles, e_halo, h_r, h_c, jnp.where(lane == 0, shifted, shifted_halo), fid[tiles, here] * img[tiles, here])
        return fit, tv

    zero = jnp.zeros((BR, TW), jnp.float32)
    total = zero
    for k in range(ITERS):
        acc = zero, zero
        if k < ITERS - 1:
            for start in range(-BR // 2, rows, BR):
                acc = sweep(k, start, acc)
        else:
            sweep(k, -BR, acc, only_duals=True)
            for b in range(blocks):
                acc = sweep(k, b * BR, acc)
                if b:
                    send(b - 1).start()
        fit, tv = acc
        total = jnp.where(lane == k, jnp.sum((0.5 / tau_step) * fit + tv_weight * tv), total)
    send(blocks - 1).start()
    partial[...] = total
    for b in range(blocks):
        send(b).wait()


def lookup_kernel(blocks, where_, owner, senders):
    def body(sender, found):
        mine = owner[sender * blocks] == where_[0]
        for i in range(1, blocks):
            mine |= owner[sender * blocks + i] == where_[0]
        senders[found] = sender
        return found + mine.astype(jnp.int32)

    lax.fori_loop(0, owner.shape[0] // blocks, body, jnp.int32(0))


def place_kernel(blocks, pixels, senders, arrived, *refs):
    parts, (out, objective, sums, sem) = refs[:-4], refs[-4:]
    copies = [
        pltpu.make_async_copy(arrived.at[senders[k]], out.at[pl.ds(k * BR, BR)], sem.at[k]) for k in range(blocks)
    ]
    for copy in copies:
        copy.start()
    values = [part[...] for part in parts]
    while len(values) > 1:
        values = [a + b for a, b in zip(values[::2], values[1::2])]
    lane = lax.broadcasted_iota(jnp.int32, values[0].shape, 1)
    for k in range(ITERS):
        sums[k] = jnp.sum(jnp.where(lane == k, values[0], 0.0)) / pixels
    copies.append(pltpu.make_async_copy(sums, objective, sem.at[blocks]))
    copies[-1].start()
    for copy in copies:
        copy.wait()


def per_device(image, cloud_mask, tile_weight, owner):
    rows_here, width_here = image.shape
    blocks, tiles = rows_here // BR, width_here // TW
    row_count, col_count = lax.axis_size(ROWS), lax.axis_size(COLS)
    height, width = rows_here * row_count, width_here * col_count
    own_row, own_col = lax.axis_index(ROWS), lax.axis_index(COLS)
    where_ = jnp.stack([own_row, own_col]).astype(jnp.int32)
    smem, vmem, hbm, anywhere = (pl.BlockSpec(memory_space=s) for s in (pltpu.SMEM, pltpu.VMEM, pltpu.HBM, pl.ANY))

    def shape(*dims):
        return jax.ShapeDtypeStruct(dims, jnp.float32)

    def work(flops):
        return pl.CostEstimate(flops=flops, bytes_accessed=0, transcendentals=0)

    def swap(array, axis, first):
        pairs = [(i, i + 1) for i in range(first, lax.axis_size(axis) - 1, 2)]
        return lax.ppermute(array, axis, pairs + [(j, i) for i, j in pairs])

    edge = shape(tiles + 1, BR, TW)
    side_a, side_b, up, down = pl.pallas_call(
        functools.partial(sides_kernel, tiles),
        in_specs=[smem, hbm, hbm],
        out_specs=[vmem] * 4,
        out_shape=[shape(BR, TW)] * 2 + [edge] * 2,
        scratch_shapes=[
            pltpu.VMEM((2, rows_here, TW), jnp.float32),
            pltpu.VMEM((2, rows_here, TW), jnp.int32),
            pltpu.VMEM((2, BR, width_here), jnp.float32),
            pltpu.VMEM((2, BR, width_here), jnp.int32),
            pltpu.SemaphoreType.DMA((8,)),
        ],
        cost_estimate=work(2 * 10**9),
        compiler_params=vmem_grant(53.5),
        name="sides",
    )(pltpu.with_memory_space_constraint(tile_weight, pltpu.HBM), image, cloud_mask)
    side_a, side_b = swap(side_a, COLS, 0), swap(side_b, COLS, 1)
    edge_b, edge_a = pl.pallas_call(
        functools.partial(corners_kernel, tiles, blocks),
        in_specs=[vmem] * 4,
        out_specs=[vmem] * 2,
        out_shape=[edge] * 2,
        cost_estimate=work(2 * 10**9),
        compiler_params=vmem_grant(2),
        name="corners",
    )(side_a, side_b, up, down)
    edge_b, edge_a = swap(edge_b, ROWS, 1), swap(edge_a, ROWS, 0)
    slots, partial = pl.pallas_call(
        functools.partial(solve_kernel, tiles, blocks, height, width),
        in_specs=[smem] * 3 + [vmem] * 6,
        out_specs=[hbm, vmem],
        out_shape=[shape(row_count, BR, width_here), shape(BR, TW)],
        scratch_shapes=[pltpu.VMEM((tiles + 1, PAD + rows_here + PAD, TW), jnp.float32)] * 7
        + [pltpu.VMEM((blocks, BR, width_here), jnp.float32), pltpu.SemaphoreType.DMA((blocks,))],
        compiler_params=vmem_grant(52),
        name="solve",
    )(where_, owner, tile_weight, image, cloud_mask, edge_b, edge_a, side_a, side_b)
    arrived = lax.all_to_all(slots, ROWS, split_axis=0, concat_axis=0, tiled=True)

    later, _ = lax.optimization_barrier((owner, partial))
    senders = pl.pallas_call(
        functools.partial(lookup_kernel, blocks),
        in_specs=[smem, smem],
        out_specs=smem,
        out_shape=jax.ShapeDtypeStruct((2 * blocks,), jnp.int32),
        compiler_params=vmem_grant(1),
        name="lookup",
    )(where_, later)

    devices = row_count * col_count

    def swapped(array, mask):
        return lax.ppermute(array, (ROWS, COLS), [(i, i ^ mask) for i in range(devices)])

    total = partial[:1]
    for bit in (1 << i for i in range(devices.bit_length() - 1)):
        if bit not in ALONG_Z:
            total = total + swapped(total, bit)
    masks = [0]
    for bit in ALONG_Z:
        masks += [mask | bit for mask in masks]
    parts = [total] + [swapped(total, mask) for mask in masks[1:]]

    solution, objective = pl.pallas_call(
        functools.partial(place_kernel, blocks, height * width),
        in_specs=[smem, anywhere] + [vmem] * len(parts),
        out_specs=[anywhere, anywhere],
        out_shape=[shape(rows_here, width_here), shape(ITERS)],
        scratch_shapes=[pltpu.SMEM((ITERS,), jnp.float32), pltpu.SemaphoreType.DMA((blocks + 1,))],
        compiler_params=vmem_grant(1),
        name="place",
    )(senders, arrived, *parts)
    return solution, objective


def solution(mesh):
    placed = (P(ROWS, COLS), P(ROWS, COLS), P(ROWS, COLS), P())
    return jax.shard_map(per_device, mesh=mesh, in_specs=placed, out_specs=(P(ROWS, COLS), P()), check_vma=False)
```

```python
import functools

import jax
import jax.numpy as jnp
from jax import lax
from jax.experimental import pallas as pl
from jax.experimental.pallas import tpu as pltpu
from jax.sharding import PartitionSpec as P

BR = 8
TW = 128
ITERS = 3
HALF = TW // 2
SIDE = 8
PAD = 16
ROWS, COLS = "rows", "cols"
ALONG_Z = (1, 16, 32)

fidelity_scale = 0.25
tau_step = 0.35
sigma_step = 0.35
tv_weight = 0.3


def vmem_grant(mebibytes):
    return pltpu.CompilerParams(vmem_limit_bytes=int(mebibytes * 2**20))


def tile_fidelity(weight, mask):
    return (tau_step * fidelity_scale * weight.astype(jnp.float32)) * (1 - mask).astype(jnp.float32)


def turned(tile, shift):
    return pltpu.roll(tile, shift % TW, 1) if shift % TW else tile


def sides_kernel(tiles, weights, image, mask, swap_a, swap_b, up, down, weight, img, msk, img_rows, msk_rows, sem):
    rows = image.shape[0]
    blocks = rows // BR
    lane = lax.broadcasted_iota(jnp.int32, (BR, TW), 1)
    sub = lax.broadcasted_iota(jnp.int32, (BR, TW), 0)
    copies = [pltpu.make_async_copy(weights, weight, sem.at[0])]
    for side in range(2):
        column, row = pl.ds(side * (tiles - 1) * TW, TW), pl.ds(side * (rows - BR), BR)
        for source, kept, kept_rows in ((image, img, img_rows), (mask, msk, msk_rows)):
            copies.append(pltpu.make_async_copy(source.at[:, column], kept.at[side], sem.at[len(copies)]))
            copies.append(pltpu.make_async_copy(source.at[row], kept_rows.at[side], sem.at[len(copies)]))
    for copy in copies:
        copy.start()
    for copy in copies:
        copy.wait()
    to_left = to_right = jnp.zeros((BR, TW), jnp.float32)
    for b in range(blocks):
        here = slice(b * BR, (b + 1) * BR)
        at = b * 2 * SIDE
        for shift, value in ((at, img[0, here]), (at + SIDE, tile_fidelity(weight[b, 0], msk[0, here]))):
            to_left = jnp.where((lane >= shift) & (lane < shift + SIDE), turned(value, shift), to_left)
        for shift, value in ((at, img[1, here]), (at + SIDE, tile_fidelity(weight[b, tiles - 1], msk[1, here]))):
            to_right = jnp.where((lane >= shift) & (lane < shift + SIDE), turned(value, shift + SIDE), to_right)
    even = lax.rem(lax.axis_index(COLS), 2) == 0
    swap_a[...] = jnp.where(even, to_right, to_left)
    swap_b[...] = jnp.where(even, to_left, to_right)
    for t in range(tiles):
        cols = slice(t * TW, (t + 1) * TW)
        f = tile_fidelity(weight[0, t], msk_rows[0, :, cols])
        up[t] = jnp.where(sub < 4, img_rows[0, :, cols], pltpu.roll(f, 4, 0))
        f = tile_fidelity(weight[blocks - 1, t], msk_rows[1, :, cols])
        down[t] = jnp.where(sub < 4, pltpu.roll(img_rows[1, :, cols], 4, 0), f)


def halo_tile(even, side_a, side_b, block):
    lane = lax.broadcasted_iota(jnp.int32, (BR, TW), 1)
    a, b = side_a[...], side_b[...]
    right, left = jnp.where(even, a, b), jnp.where(even, b, a)
    at = block * 2 * SIDE

    def spread(at):
        return jnp.where(lane < HALF, turned(right, -at), turned(left, -at - SIDE))

    return spread(at), spread(at + SIDE)


def corners_kernel(tiles, blocks, side_a, side_b, up, down, swap_b, swap_a):
    sub = lax.broadcasted_iota(jnp.int32, (BR, TW), 0)
    even_col = lax.rem(lax.axis_index(COLS), 2) == 0
    even_row = lax.rem(lax.axis_index(ROWS), 2) == 0

    def put(t, top, bottom):
        swap_a[t] = jnp.where(even_row, bottom, top)
        swap_b[t] = jnp.where(even_row, top, bottom)

    for t in range(tiles):
        put(t, up[t], down[t])
    g, f = halo_tile(even_col, side_a, side_b, 0)
    top = jnp.where(sub < 4, g, pltpu.roll(f, 4, 0))
    g, f = halo_tile(even_col, side_a, side_b, blocks - 1)
    put(tiles, top, jnp.where(sub < 4, pltpu.roll(g, 4, 0), f))


def solve_kernel(
    tiles, blocks, height, width,
    owners, weights, image, mask, edge_b, edge_a, side_a, side_b,
    slots, partial,
    owner, weight, img, fid, inv, ext, pri, dual_r, dual_c, staged, sem,
):
    rows = blocks * BR
    fetch_owner = pltpu.make_async_copy(owners, owner, sem.at[blocks])
    fetch_weight = pltpu.make_async_copy(weights, weight, sem.at[blocks + 1])
    fetch_owner.start()
    fetch_weight.start()
    own_row, own_col = lax.axis_index(ROWS), lax.axis_index(COLS)
    even_row, even_col = lax.rem(own_row, 2) == 0, lax.rem(own_col, 2) == 0
    lane = lax.broadcasted_iota(jnp.int32, (BR, TW), 1)
    sub = lax.broadcasted_iota(jnp.int32, (BR, TW), 0)

    low, high = slice(PAD - BR, PAD), slice(PAD + rows, PAD + rows + BR)
    for t in range(tiles + 1):
        a, b = edge_a[t], edge_b[t]
        v, w = jnp.where(even_row, b, a), jnp.where(even_row, a, b)
        for at, g, f in (
            (low, jnp.where(sub >= 4, pltpu.roll(v, 4, 0), 0.0), jnp.where(sub >= 4, v, 0.0)),
            (high, jnp.where(sub < 4, w, 0.0), jnp.where(sub < 4, pltpu.roll(w, 4, 0), 0.0)),
        ):
            img[t, at] = g
            fid[t, at] = f
            inv[t, at] = 1.0 / (1.0 + f)
    for b in range(blocks):
        here = slice(PAD + b * BR, PAD + (b + 1) * BR)
        g, f = halo_tile(even_col, side_a, side_b, b)
        img[tiles, here] = g
        fid[tiles, here] = f
        inv[tiles, here] = 1.0 / (1.0 + f)
    fetch_weight.wait()
    for t in range(tiles):
        for b in range(blocks):
            natural, cols = slice(b * BR, (b + 1) * BR), slice(t * TW, (t + 1) * TW)
            here = slice(PAD + b * BR, PAD + (b + 1) * BR)
            f = tile_fidelity(weight[b, t], mask[natural, cols])
            img[t, here] = image[natural, cols]
            fid[t, here] = f
            inv[t, here] = 1.0 / (1.0 + f)

    col = own_col * (tiles * TW) + lane
    inner_last = col + (tiles - 1) * TW < width - 1
    halo_col = jnp.where(lane < HALF, col + tiles * TW, col - TW)
    inner_halo = (halo_col >= 0) & (halo_col < width - 1)

    def send(b):
        return pltpu.make_async_copy(staged.at[b], slots.at[owner[own_row * blocks + b]], sem.at[b])

    def sweep(k, start, acc, only_duals=False):
        base = PAD + start
        here, lower, upper = pl.ds(base, BR), pl.ds(base + 1, BR), pl.ds(base - 1, BR)
        first, final = k == 0, k == ITERS - 1
        source = img if first else ext
        row = own_row * rows + start + sub
        inner_row = (row >= 0) & (row < height - 1)

        def duals(t, e, right):
            g_r = source[t, lower] - e
            if start < 0 or start + BR >= rows:
                g_r = jnp.where(inner_row, g_r, 0.0)
            g_c = right - e
            if t == tiles - 1:
                g_c = jnp.where(inner_last, g_c, 0.0)
            if t == tiles:
                g_c = jnp.where(inner_halo, g_c, 0.0)
            n = g_r * g_r + g_c * g_c
            s = lax.rsqrt(n)
            steep = jnp.where(n > 0.0, n * s, 0.0)
            q_r, q_c = g_r, g_c
            if not first:
                q_r, q_c = dual_r[t, here] + q_r, dual_c[t, here] + q_c
                s = lax.rsqrt(q_r * q_r + q_c * q_c)
            scale = jnp.minimum(1.0, (tv_weight / sigma_step) * s)
            d_r, d_c = q_r * scale, q_c * scale
            dual_r[t, here] = d_r
            if not final:
                dual_c[t, here] = d_c
            return steep, d_r, d_c

        def update(t, e, d_r, d_c, left, pull):
            div = d_r - dual_r[t, upper] + (d_c - left)
            p = e if first else pri[t, here]
            u = (p + (tau_step * sigma_step) * div + pull) * inv[t, here]
            if final:
                staged[start // BR, :, t * TW:(t + 1) * TW] = u
            else:
                ext[t, here] = u + (u - p)
                pri[t, here] = u
            return u

        e_halo = source[tiles, here]
        e = source[0, here]
        turned = pltpu.roll(e, TW - 1, 1)
        turned_halo = pltpu.roll(e_halo, TW - 1, 1)
        _, h_r, h_c = duals(tiles, e_halo, jnp.where(lane == TW - 1, turned, turned_halo))
        shifted = pltpu.roll(h_c, 1, 1)
        shifted_halo = shifted
        fit, tv = acc
        for t in range(tiles):
            if t < tiles - 1:
                e_next = source[t + 1, here]
                turned_next = pltpu.roll(e_next, TW - 1, 1)
            else:
                e_next, turned_next = None, turned_halo
            steep, d_r, d_c = duals(t, e, jnp.where(lane == TW - 1, turned_next, turned))
            if only_duals:
                e, turned = e_next, turned_next
                continue
            shifted_here = pltpu.roll(d_c, 1, 1)
            g, f = img[t, here], fid[t, here]
            u = update(t, e, d_r, d_c, jnp.where(lane == 0, shifted, shifted_here), f * g)
            miss = u - g
            loss = f * (miss * miss)
            if start < 0:
                loss, steep = jnp.where(sub >= -start, loss, 0.0), jnp.where(sub >= -start, steep, 0.0)
            elif start + BR > rows:
                loss, steep = jnp.where(sub < rows - start, loss, 0.0), jnp.where(sub < rows - start, steep, 0.0)
            fit, tv = fit + loss, tv + steep
            shifted, e, turned = shifted_here, e_next, turned_next
        if not final:
            update(tiles, e_halo, h_r, h_c, jnp.where(lane == 0, shifted, shifted_halo), fid[tiles, here] * img[tiles, here])
        return fit, tv

    zero = jnp.zeros((BR, TW), jnp.float32)
    total = zero
    for k in range(ITERS):
        acc = zero, zero
        if k < ITERS - 1:
            for start in range(-BR // 2, rows, BR):
                acc = sweep(k, start, acc)
        else:
            sweep(k, -BR, acc, only_duals=True)
            fetch_owner.wait()
            for b in range(blocks):
                acc = sweep(k, b * BR, acc)
                if b:
                    send(b - 1).start()
        fit, tv = acc
        total = jnp.where(lane == k, jnp.sum((0.5 / tau_step) * fit + tv_weight * tv), total)
    send(blocks - 1).start()
    partial[...] = total
    for b in range(blocks):
        send(b).wait()


def lookup_kernel(blocks, owner, senders):
    own_row = lax.axis_index(ROWS)

    def body(sender, found):
        mine = owner[sender * blocks] == own_row
        for i in range(1, blocks):
            mine |= owner[sender * blocks + i] == own_row
        senders[found] = sender
        return found + mine.astype(jnp.int32)

    lax.fori_loop(0, owner.shape[0] // blocks, body, jnp.int32(0))


def place_kernel(blocks, pixels, senders, arrived, *refs):
    parts, (out, objective, sums, sem) = refs[:-4], refs[-4:]
    copies = [
        pltpu.make_async_copy(arrived.at[senders[k]], out.at[pl.ds(k * BR, BR)], sem.at[k]) for k in range(blocks)
    ]
    for copy in copies:
        copy.start()
    values = [part[...] for part in parts]
    while len(values) > 1:
        values = [a + b for a, b in zip(values[::2], values[1::2])]
    lane = lax.broadcasted_iota(jnp.int32, values[0].shape, 1)
    for k in range(ITERS):
        sums[k] = jnp.sum(jnp.where(lane == k, values[0], 0.0)) / pixels
    copies.append(pltpu.make_async_copy(sums, objective, sem.at[blocks]))
    copies[-1].start()
    for copy in copies:
        copy.wait()


def per_device(image, cloud_mask, tile_weight, owner):
    rows_here, width_here = image.shape
    blocks, tiles = rows_here // BR, width_here // TW
    row_count, col_count = lax.axis_size(ROWS), lax.axis_size(COLS)
    height, width = rows_here * row_count, width_here * col_count
    smem, vmem, hbm, anywhere = (pl.BlockSpec(memory_space=s) for s in (pltpu.SMEM, pltpu.VMEM, pltpu.HBM, pl.ANY))

    def shape(*dims):
        return jax.ShapeDtypeStruct(dims, jnp.float32)

    def work(flops):
        return pl.CostEstimate(flops=flops, bytes_accessed=0, transcendentals=0)

    def swap(array, axis, first):
        pairs = [(i, i + 1) for i in range(first, lax.axis_size(axis) - 1, 2)]
        return lax.ppermute(array, axis, pairs + [(j, i) for i, j in pairs])

    edge = shape(tiles + 1, BR, TW)
    side_a, side_b, up, down = pl.pallas_call(
        functools.partial(sides_kernel, tiles),
        in_specs=[hbm] * 3,
        out_specs=[vmem] * 4,
        out_shape=[shape(BR, TW)] * 2 + [edge] * 2,
        scratch_shapes=[
            pltpu.SMEM(tile_weight.shape, jnp.int32),
            pltpu.VMEM((2, rows_here, TW), jnp.float32),
            pltpu.VMEM((2, rows_here, TW), jnp.int32),
            pltpu.VMEM((2, BR, width_here), jnp.float32),
            pltpu.VMEM((2, BR, width_here), jnp.int32),
            pltpu.SemaphoreType.DMA((9,)),
        ],
        cost_estimate=work(2 * 10**9),
        compiler_params=vmem_grant(53.5),
        name="sides",
    )(pltpu.with_memory_space_constraint(tile_weight, pltpu.HBM), image, cloud_mask)
    side_a, side_b = swap(side_a, COLS, 0), swap(side_b, COLS, 1)
    edge_b, edge_a = pl.pallas_call(
        functools.partial(corners_kernel, tiles, blocks),
        in_specs=[vmem] * 4,
        out_specs=[vmem] * 2,
        out_shape=[edge] * 2,
        cost_estimate=work(2 * 10**9),
        compiler_params=vmem_grant(2),
        name="corners",
    )(side_a, side_b, up, down)
    edge_b, edge_a = swap(edge_b, ROWS, 1), swap(edge_a, ROWS, 0)
    slots, partial = pl.pallas_call(
        functools.partial(solve_kernel, tiles, blocks, height, width),
        in_specs=[anywhere] * 2 + [vmem] * 6,
        out_specs=[hbm, vmem],
        out_shape=[shape(row_count, BR, width_here), shape(BR, TW)],
        scratch_shapes=[pltpu.SMEM(owner.shape, jnp.int32), pltpu.SMEM(tile_weight.shape, jnp.int32)]
        + [pltpu.VMEM((tiles + 1, PAD + rows_here + PAD, TW), jnp.float32)] * 7
        + [pltpu.VMEM((blocks, BR, width_here), jnp.float32), pltpu.SemaphoreType.DMA((blocks + 2,))],
        compiler_params=vmem_grant(52),
        name="solve",
    )(owner, tile_weight, image, cloud_mask, edge_b, edge_a, side_a, side_b)
    arrived = lax.all_to_all(slots, ROWS, split_axis=0, concat_axis=0, tiled=True)

    later, _ = lax.optimization_barrier((owner, partial))
    senders = pl.pallas_call(
        functools.partial(lookup_kernel, blocks),
        in_specs=[smem],
        out_specs=smem,
        out_shape=jax.ShapeDtypeStruct((2 * blocks,), jnp.int32),
        compiler_params=vmem_grant(1),
        name="lookup",
    )(later)

    devices = row_count * col_count

    def swapped(array, mask):
        return lax.ppermute(array, (ROWS, COLS), [(i, i ^ mask) for i in range(devices)])

    total = partial[:1]
    for bit in (1 << i for i in range(devices.bit_length() - 1)):
        if bit not in ALONG_Z:
            total = total + swapped(total, bit)
    masks = [0]
    for bit in ALONG_Z:
        masks += [mask | bit for mask in masks]
    parts = [total] + [swapped(total, mask) for mask in masks[1:]]

    solution, objective = pl.pallas_call(
        functools.partial(place_kernel, blocks, height * width),
        in_specs=[smem, anywhere] + [vmem] * len(parts),
        out_specs=[anywhere, anywhere],
        out_shape=[shape(rows_here, width_here), shape(ITERS)],
        scratch_shapes=[pltpu.SMEM((ITERS,), jnp.float32), pltpu.SemaphoreType.DMA((blocks + 1,))],
        compiler_params=vmem_grant(1),
        name="place",
    )(senders, arrived, *parts)
    return solution, objective


def solution(mesh):
    placed = (P(ROWS, COLS), P(ROWS, COLS), P(ROWS, COLS), P())
    return jax.shard_map(per_device, mesh=mesh, in_specs=placed, out_specs=(P(ROWS, COLS), P()), check_vma=False)
```

```python
import functools

import jax
import jax.numpy as jnp
from jax import lax
from jax.experimental import pallas as pl
from jax.experimental.pallas import tpu as pltpu
from jax.sharding import PartitionSpec as P

BR = 8
TW = 128
ITERS = 3
HALF = TW // 2
SIDE = 8
PAD = 16
ROWS, COLS = "rows", "cols"
ALONG_Z = (1, 16, 32)

fidelity_scale = 0.25
tau_step = 0.35
sigma_step = 0.35
tv_weight = 0.3


def vmem_grant(mebibytes):
    return pltpu.CompilerParams(vmem_limit_bytes=int(mebibytes * 2**20))


def tile_fidelity(weight, mask):
    return (tau_step * fidelity_scale * weight.astype(jnp.float32)) * (1 - mask).astype(jnp.float32)


def turned(tile, shift):
    return pltpu.roll(tile, shift % TW, 1) if shift % TW else tile


def sides_kernel(tiles, weights, image, mask, swap_b, swap_a, up, down, weight, img, msk, img_rows, msk_rows, sem):
    rows = image.shape[0]
    blocks = rows // BR
    lane = lax.broadcasted_iota(jnp.int32, (BR, TW), 1)
    sub = lax.broadcasted_iota(jnp.int32, (BR, TW), 0)
    copies = [pltpu.make_async_copy(weights, weight, sem.at[0])]
    for side in range(2):
        column, row = pl.ds(side * (tiles - 1) * TW, TW), pl.ds(side * (rows - BR), BR)
        for source, kept, kept_rows in ((image, img, img_rows), (mask, msk, msk_rows)):
            copies.append(pltpu.make_async_copy(source.at[:, column], kept.at[side], sem.at[len(copies)]))
            copies.append(pltpu.make_async_copy(source.at[row], kept_rows.at[side], sem.at[len(copies)]))
    for copy in copies:
        copy.start()
    for copy in copies:
        copy.wait()
    to_left = to_right = jnp.zeros((BR, TW), jnp.float32)
    for b in range(blocks):
        here = slice(b * BR, (b + 1) * BR)
        at = b * 2 * SIDE
        for shift, value in ((at, img[0, here]), (at + SIDE, tile_fidelity(weight[b, 0], msk[0, here]))):
            to_left = jnp.where((lane >= shift) & (lane < shift + SIDE), turned(value, shift), to_left)
        for shift, value in ((at, img[1, here]), (at + SIDE, tile_fidelity(weight[b, tiles - 1], msk[1, here]))):
            to_right = jnp.where((lane >= shift) & (lane < shift + SIDE), turned(value, shift + SIDE), to_right)
    even = lax.rem(lax.axis_index(COLS), 2) == 0
    swap_a[...] = jnp.where(even, to_right, to_left)
    swap_b[...] = jnp.where(even, to_left, to_right)
    for t in range(tiles):
        cols = slice(t * TW, (t + 1) * TW)
        f = tile_fidelity(weight[0, t], msk_rows[0, :, cols])
        up[t] = jnp.where(sub < 4, img_rows[0, :, cols], pltpu.roll(f, 4, 0))
        f = tile_fidelity(weight[blocks - 1, t], msk_rows[1, :, cols])
        down[t] = jnp.where(sub < 4, pltpu.roll(img_rows[1, :, cols], 4, 0), f)


def halo_tile(even, side_a, side_b, block):
    lane = lax.broadcasted_iota(jnp.int32, (BR, TW), 1)
    a, b = side_a[...], side_b[...]
    right, left = jnp.where(even, a, b), jnp.where(even, b, a)
    at = block * 2 * SIDE

    def spread(at):
        return jnp.where(lane < HALF, turned(right, -at), turned(left, -at - SIDE))

    return spread(at), spread(at + SIDE)


def corners_kernel(tiles, blocks, side_b, side_a, up, down, swap_b, swap_a):
    sub = lax.broadcasted_iota(jnp.int32, (BR, TW), 0)
    even_col = lax.rem(lax.axis_index(COLS), 2) == 0
    even_row = lax.rem(lax.axis_index(ROWS), 2) == 0

    def put(t, top, bottom):
        swap_a[t] = jnp.where(even_row, bottom, top)
        swap_b[t] = jnp.where(even_row, top, bottom)

    for t in range(tiles):
        put(t, up[t], down[t])
    g, f = halo_tile(even_col, side_a, side_b, 0)
    top = jnp.where(sub < 4, g, pltpu.roll(f, 4, 0))
    g, f = halo_tile(even_col, side_a, side_b, blocks - 1)
    put(tiles, top, jnp.where(sub < 4, pltpu.roll(g, 4, 0), f))


def solve_kernel(
    tiles, blocks, height, width,
    owners, weights, image, mask, edge_b, edge_a, side_b, side_a,
    slots, partial,
    owner, weight, img, fid, inv, ext, pri, dual_r, dual_c, staged, sem,
):
    rows = blocks * BR
    fetch_owner = pltpu.make_async_copy(owners, owner, sem.at[blocks])
    fetch_weight = pltpu.make_async_copy(weights, weight, sem.at[blocks + 1])
    fetch_owner.start()
    fetch_weight.start()
    own_row, own_col = lax.axis_index(ROWS), lax.axis_index(COLS)
    even_row, even_col = lax.rem(own_row, 2) == 0, lax.rem(own_col, 2) == 0
    lane = lax.broadcasted_iota(jnp.int32, (BR, TW), 1)
    sub = lax.broadcasted_iota(jnp.int32, (BR, TW), 0)

    low, high = slice(PAD - BR, PAD), slice(PAD + rows, PAD + rows + BR)
    for t in range(tiles + 1):
        a, b = edge_a[t], edge_b[t]
        v, w = jnp.where(even_row, b, a), jnp.where(even_row, a, b)
        for at, g, f in (
            (low, jnp.where(sub >= 4, pltpu.roll(v, 4, 0), 0.0), jnp.where(sub >= 4, v, 0.0)),
            (high, jnp.where(sub < 4, w, 0.0), jnp.where(sub < 4, pltpu.roll(w, 4, 0), 0.0)),
        ):
            img[t, at] = g
            fid[t, at] = f
            inv[t, at] = 1.0 / (1.0 + f)
    for b in range(blocks):
        here = slice(PAD + b * BR, PAD + (b + 1) * BR)
        g, f = halo_tile(even_col, side_a, side_b, b)
        img[tiles, here] = g
        fid[tiles, here] = f
        inv[tiles, here] = 1.0 / (1.0 + f)
    fetch_weight.wait()
    for t in range(tiles):
        for b in range(blocks):
            natural, cols = slice(b * BR, (b + 1) * BR), slice(t * TW, (t + 1) * TW)
            here = slice(PAD + b * BR, PAD + (b + 1) * BR)
            f = tile_fidelity(weight[b, t], mask[natural, cols])
            img[t, here] = image[natural, cols]
            fid[t, here] = f
            inv[t, here] = 1.0 / (1.0 + f)

    col = own_col * (tiles * TW) + lane
    inner_last = col + (tiles - 1) * TW < width - 1
    halo_col = jnp.where(lane < HALF, col + tiles * TW, col - TW)
    inner_halo = (halo_col >= 0) & (halo_col < width - 1)

    def send(b):
        return pltpu.make_async_copy(staged.at[b], slots.at[owner[own_row * blocks + b]], sem.at[b])

    def sweep(k, start, acc, only_duals=False):
        base = PAD + start
        here, lower, upper = pl.ds(base, BR), pl.ds(base + 1, BR), pl.ds(base - 1, BR)
        first, final = k == 0, k == ITERS - 1
        source = img if first else ext
        row = own_row * rows + start + sub
        inner_row = (row >= 0) & (row < height - 1)

        def duals(t, e, right):
            g_r = source[t, lower] - e
            if start < 0 or start + BR >= rows:
                g_r = jnp.where(inner_row, g_r, 0.0)
            g_c = right - e
            if t == tiles - 1:
                g_c = jnp.where(inner_last, g_c, 0.0)
            if t == tiles:
                g_c = jnp.where(inner_halo, g_c, 0.0)
            n = g_r * g_r + g_c * g_c
            s = lax.rsqrt(n)
            steep = jnp.where(n > 0.0, n * s, 0.0)
            q_r, q_c = g_r, g_c
            if not first:
                q_r, q_c = dual_r[t, here] + q_r, dual_c[t, here] + q_c
                s = lax.rsqrt(q_r * q_r + q_c * q_c)
            scale = jnp.minimum(1.0, (tv_weight / sigma_step) * s)
            d_r, d_c = q_r * scale, q_c * scale
            dual_r[t, here] = d_r
            if not final:
                dual_c[t, here] = d_c
            return steep, d_r, d_c

        def update(t, e, d_r, d_c, left, pull):
            div = d_r - dual_r[t, upper] + (d_c - left)
            p = e if first else pri[t, here]
            u = (p + (tau_step * sigma_step) * div + pull) * inv[t, here]
            if final:
                staged[start // BR, :, t * TW:(t + 1) * TW] = u
            else:
                ext[t, here] = u + (u - p)
                pri[t, here] = u
            return u

        e_halo = source[tiles, here]
        e = source[0, here]
        turned = pltpu.roll(e, TW - 1, 1)
        turned_halo = pltpu.roll(e_halo, TW - 1, 1)
        _, h_r, h_c = duals(tiles, e_halo, jnp.where(lane == TW - 1, turned, turned_halo))
        shifted = pltpu.roll(h_c, 1, 1)
        shifted_halo = shifted
        fit, tv = acc
        for t in range(tiles):
            if t < tiles - 1:
                e_next = source[t + 1, here]
                turned_next = pltpu.roll(e_next, TW - 1, 1)
            else:
                e_next, turned_next = None, turned_halo
            steep, d_r, d_c = duals(t, e, jnp.where(lane == TW - 1, turned_next, turned))
            if only_duals:
                e, turned = e_next, turned_next
                continue
            shifted_here = pltpu.roll(d_c, 1, 1)
            g, f = img[t, here], fid[t, here]
            u = update(t, e, d_r, d_c, jnp.where(lane == 0, shifted, shifted_here), f * g)
            miss = u - g
            loss = f * (miss * miss)
            if start < 0:
                loss, steep = jnp.where(sub >= -start, loss, 0.0), jnp.where(sub >= -start, steep, 0.0)
            elif start + BR > rows:
                loss, steep = jnp.where(sub < rows - start, loss, 0.0), jnp.where(sub < rows - start, steep, 0.0)
            fit, tv = fit + loss, tv + steep
            shifted, e, turned = shifted_here, e_next, turned_next
        if not final:
            update(tiles, e_halo, h_r, h_c, jnp.where(lane == 0, shifted, shifted_halo), fid[tiles, here] * img[tiles, here])
        return fit, tv

    zero = jnp.zeros((BR, TW), jnp.float32)
    total = zero
    for k in range(ITERS):
        acc = zero, zero
        if k < ITERS - 1:
            for start in range(-BR // 2, rows, BR):
                acc = sweep(k, start, acc)
        else:
            sweep(k, -BR, acc, only_duals=True)
            fetch_owner.wait()
            for b in range(blocks):
                acc = sweep(k, b * BR, acc)
                if b:
                    send(b - 1).start()
        fit, tv = acc
        total = jnp.where(lane == k, jnp.sum((0.5 / tau_step) * fit + tv_weight * tv), total)
    send(blocks - 1).start()
    partial[...] = total
    for b in range(blocks):
        send(b).wait()


def lookup_kernel(blocks, owner, senders):
    own_row = lax.axis_index(ROWS)

    def body(sender, found):
        mine = owner[sender * blocks] == own_row
        for i in range(1, blocks):
            mine |= owner[sender * blocks + i] == own_row
        senders[found] = sender
        return found + mine.astype(jnp.int32)

    lax.fori_loop(0, owner.shape[0] // blocks, body, jnp.int32(0))


def place_kernel(blocks, pixels, senders, arrived, *refs):
    parts, (out, objective, sums, sem) = refs[:-4], refs[-4:]
    copies = [
        pltpu.make_async_copy(arrived.at[senders[k]], out.at[pl.ds(k * BR, BR)], sem.at[k]) for k in range(blocks)
    ]
    for copy in copies:
        copy.start()
    values = [part[...] for part in parts]
    while len(values) > 1:
        values = [a + b for a, b in zip(values[::2], values[1::2])]
    lane = lax.broadcasted_iota(jnp.int32, values[0].shape, 1)
    for k in range(ITERS):
        sums[k] = jnp.sum(jnp.where(lane == k, values[0], 0.0)) / pixels
    copies.append(pltpu.make_async_copy(sums, objective, sem.at[blocks]))
    copies[-1].start()
    for copy in copies:
        copy.wait()


def per_device(image, cloud_mask, tile_weight, owner):
    rows_here, width_here = image.shape
    blocks, tiles = rows_here // BR, width_here // TW
    row_count, col_count = lax.axis_size(ROWS), lax.axis_size(COLS)
    height, width = rows_here * row_count, width_here * col_count
    smem, vmem, hbm, anywhere = (pl.BlockSpec(memory_space=s) for s in (pltpu.SMEM, pltpu.VMEM, pltpu.HBM, pl.ANY))

    def shape(*dims):
        return jax.ShapeDtypeStruct(dims, jnp.float32)

    def work(flops):
        return pl.CostEstimate(flops=flops, bytes_accessed=0, transcendentals=0)

    def swap(array, axis, first):
        pairs = [(i, i + 1) for i in range(first, lax.axis_size(axis) - 1, 2)]
        return lax.ppermute(array, axis, pairs + [(j, i) for i, j in pairs])

    edge = shape(tiles + 1, BR, TW)
    side_b, side_a, up, down = pl.pallas_call(
        functools.partial(sides_kernel, tiles),
        in_specs=[hbm] * 3,
        out_specs=[vmem] * 4,
        out_shape=[shape(BR, TW)] * 2 + [edge] * 2,
        scratch_shapes=[
            pltpu.SMEM(tile_weight.shape, jnp.int32),
            pltpu.VMEM((2, rows_here, TW), jnp.float32),
            pltpu.VMEM((2, rows_here, TW), jnp.int32),
            pltpu.VMEM((2, BR, width_here), jnp.float32),
            pltpu.VMEM((2, BR, width_here), jnp.int32),
            pltpu.SemaphoreType.DMA((9,)),
        ],
        cost_estimate=work(2 * 10**9),
        compiler_params=vmem_grant(53.5),
        name="sides",
    )(pltpu.with_memory_space_constraint(tile_weight, pltpu.HBM), image, cloud_mask)
    side_b, side_a = swap(side_b, COLS, 1), swap(side_a, COLS, 0)
    edge_b, edge_a = pl.pallas_call(
        functools.partial(corners_kernel, tiles, blocks),
        in_specs=[vmem] * 4,
        out_specs=[vmem] * 2,
        out_shape=[edge] * 2,
        cost_estimate=work(2 * 10**9),
        compiler_params=vmem_grant(2),
        name="corners",
    )(side_b, side_a, up, down)
    edge_b, edge_a = swap(edge_b, ROWS, 1), swap(edge_a, ROWS, 0)
    slots, partial = pl.pallas_call(
        functools.partial(solve_kernel, tiles, blocks, height, width),
        in_specs=[anywhere] * 2 + [vmem] * 6,
        out_specs=[hbm, vmem],
        out_shape=[shape(row_count, BR, width_here), shape(BR, TW)],
        scratch_shapes=[pltpu.SMEM(owner.shape, jnp.int32), pltpu.SMEM(tile_weight.shape, jnp.int32)]
        + [pltpu.VMEM((tiles + 1, PAD + rows_here + PAD, TW), jnp.float32)] * 7
        + [pltpu.VMEM((blocks, BR, width_here), jnp.float32), pltpu.SemaphoreType.DMA((blocks + 2,))],
        compiler_params=vmem_grant(52),
        name="solve",
    )(owner, tile_weight, image, cloud_mask, edge_b, edge_a, side_b, side_a)
    arrived = lax.all_to_all(slots, ROWS, split_axis=0, concat_axis=0, tiled=True)

    later, _ = lax.optimization_barrier((owner, partial))
    senders = pl.pallas_call(
        functools.partial(lookup_kernel, blocks),
        in_specs=[smem],
        out_specs=smem,
        out_shape=jax.ShapeDtypeStruct((2 * blocks,), jnp.int32),
        compiler_params=vmem_grant(1),
        name="lookup",
    )(later)

    devices = row_count * col_count

    def swapped(array, mask):
        return lax.ppermute(array, (ROWS, COLS), [(i, i ^ mask) for i in range(devices)])

    total = partial[:1]
    for bit in (1 << i for i in range(devices.bit_length() - 1)):
        if bit not in ALONG_Z:
            total = total + swapped(total, bit)
    masks = [0]
    for bit in ALONG_Z:
        masks += [mask | bit for mask in masks]
    parts = [total] + [swapped(total, mask) for mask in masks[1:]]

    solution, objective = pl.pallas_call(
        functools.partial(place_kernel, blocks, height * width),
        in_specs=[smem, anywhere] + [vmem] * len(parts),
        out_specs=[anywhere, anywhere],
        out_shape=[shape(rows_here, width_here), shape(ITERS)],
        scratch_shapes=[pltpu.SMEM((ITERS,), jnp.float32), pltpu.SemaphoreType.DMA((blocks + 1,))],
        compiler_params=vmem_grant(1),
        name="place",
    )(senders, arrived, *parts)
    return solution, objective


def solution(mesh):
    placed = (P(ROWS, COLS), P(ROWS, COLS), P(ROWS, COLS), P())
    return jax.shard_map(per_device, mesh=mesh, in_specs=placed, out_specs=(P(ROWS, COLS), P()), check_vma=False)
```

```python
import functools

import jax
import jax.numpy as jnp
from jax import lax
from jax.experimental import pallas as pl
from jax.experimental.pallas import tpu as pltpu
from jax.sharding import PartitionSpec as P

BR = 8
TW = 128
ITERS = 3
HALF = TW // 2
SIDE = 8
PAD = 16
ROWS, COLS = "rows", "cols"
ALONG_Z = (1, 16, 32)

fidelity_scale = 0.25
tau_step = 0.35
sigma_step = 0.35
tv_weight = 0.3


def vmem_grant(mebibytes):
    return pltpu.CompilerParams(vmem_limit_bytes=int(mebibytes * 2**20))


def tile_fidelity(weight, mask):
    return (tau_step * fidelity_scale * weight.astype(jnp.float32)) * (1 - mask).astype(jnp.float32)


def turned(tile, shift):
    return pltpu.roll(tile, shift % TW, 1) if shift % TW else tile


def sides_kernel(tiles, weights, image, mask, swap_b, swap_a, up, down, weight, img, msk, img_rows, msk_rows, sem):
    rows = image.shape[0]
    blocks = rows // BR
    lane = lax.broadcasted_iota(jnp.int32, (BR, TW), 1)
    sub = lax.broadcasted_iota(jnp.int32, (BR, TW), 0)
    copies = [pltpu.make_async_copy(weights, weight, sem.at[0])]
    for side in range(2):
        column, row = pl.ds(side * (tiles - 1) * TW, TW), pl.ds(side * (rows - BR), BR)
        for source, kept, kept_rows in ((image, img, img_rows), (mask, msk, msk_rows)):
            copies.append(pltpu.make_async_copy(source.at[:, column], kept.at[side], sem.at[len(copies)]))
            copies.append(pltpu.make_async_copy(source.at[row], kept_rows.at[side], sem.at[len(copies)]))
    for copy in copies:
        copy.start()
    for copy in copies:
        copy.wait()
    to_left = to_right = jnp.zeros((BR, TW), jnp.float32)
    for b in range(blocks):
        here = slice(b * BR, (b + 1) * BR)
        at = b * 2 * SIDE
        for shift, value in ((at, img[0, here]), (at + SIDE, tile_fidelity(weight[b, 0], msk[0, here]))):
            to_left = jnp.where((lane >= shift) & (lane < shift + SIDE), turned(value, shift), to_left)
        for shift, value in ((at, img[1, here]), (at + SIDE, tile_fidelity(weight[b, tiles - 1], msk[1, here]))):
            to_right = jnp.where((lane >= shift) & (lane < shift + SIDE), turned(value, shift + SIDE), to_right)
    even = lax.rem(lax.axis_index(COLS), 2) == 0
    swap_a[...] = jnp.where(even, to_right, to_left)
    swap_b[...] = jnp.where(even, to_left, to_right)
    for t in range(tiles):
        cols = slice(t * TW, (t + 1) * TW)
        f = tile_fidelity(weight[0, t], msk_rows[0, :, cols])
        up[t] = jnp.where(sub < 4, img_rows[0, :, cols], pltpu.roll(f, 4, 0))
        f = tile_fidelity(weight[blocks - 1, t], msk_rows[1, :, cols])
        down[t] = jnp.where(sub < 4, pltpu.roll(img_rows[1, :, cols], 4, 0), f)


def halo_tile(even, side_a, side_b, block):
    lane = lax.broadcasted_iota(jnp.int32, (BR, TW), 1)
    a, b = side_a[...], side_b[...]
    right, left = jnp.where(even, a, b), jnp.where(even, b, a)
    at = block * 2 * SIDE

    def spread(at):
        return jnp.where(lane < HALF, turned(right, -at), turned(left, -at - SIDE))

    return spread(at), spread(at + SIDE)


def corners_kernel(tiles, blocks, side_b, side_a, up, down, swap_b, swap_a):
    sub = lax.broadcasted_iota(jnp.int32, (BR, TW), 0)
    even_col = lax.rem(lax.axis_index(COLS), 2) == 0
    even_row = lax.rem(lax.axis_index(ROWS), 2) == 0

    def put(t, top, bottom):
        swap_a[t] = jnp.where(even_row, bottom, top)
        swap_b[t] = jnp.where(even_row, top, bottom)

    for t in range(tiles):
        put(t, up[t], down[t])
    g, f = halo_tile(even_col, side_a, side_b, 0)
    top = jnp.where(sub < 4, g, pltpu.roll(f, 4, 0))
    g, f = halo_tile(even_col, side_a, side_b, blocks - 1)
    put(tiles, top, jnp.where(sub < 4, pltpu.roll(g, 4, 0), f))


def sweeper(tiles, rows, height, width, slots_of, img, fid, inv, ext, pri, dual_r, dual_c):
    own_row, own_col = lax.axis_index(ROWS), lax.axis_index(COLS)
    lane = lax.broadcasted_iota(jnp.int32, (BR, TW), 1)
    sub = lax.broadcasted_iota(jnp.int32, (BR, TW), 0)
    col = own_col * (tiles * TW) + lane
    inner_last = col + (tiles - 1) * TW < width - 1
    halo_col = jnp.where(lane < HALF, col + tiles * TW, col - TW)
    inner_halo = (halo_col >= 0) & (halo_col < width - 1)

    def sweep(k, start, acc, part="all"):
        base = PAD + start
        here, lower, upper = pl.ds(base, BR), pl.ds(base + 1, BR), pl.ds(base - 1, BR)
        first, final = k == 0, k == ITERS - 1
        source = img if first else ext
        row = own_row * rows + start + sub
        inner_row = (row >= 0) & (row < height - 1)

        def ahead(t):
            return pltpu.roll(source[t, here], TW - 1, 1)

        def duals(t, right):
            e = source[t, here]
            g_r = source[t, lower] - e
            if start < 0 or start + BR >= rows:
                g_r = jnp.where(inner_row, g_r, 0.0)
            g_c = right - e
            if t == tiles - 1:
                g_c = jnp.where(inner_last, g_c, 0.0)
            if t == tiles:
                g_c = jnp.where(inner_halo, g_c, 0.0)
            n = g_r * g_r + g_c * g_c
            s = lax.rsqrt(n)
            steep = jnp.where(n > 0.0, n * s, 0.0)
            q_r, q_c = g_r, g_c
            if not first:
                q_r, q_c = dual_r[t, here] + q_r, dual_c[t, here] + q_c
                s = lax.rsqrt(q_r * q_r + q_c * q_c)
            scale = jnp.minimum(1.0, (tv_weight / sigma_step) * s)
            d_r, d_c = q_r * scale, q_c * scale
            dual_r[t, here] = d_r
            if not final:
                dual_c[t, here] = d_c
            return steep, d_r, d_c

        def update(t, d_r, d_c, left):
            div = d_r - dual_r[t, upper] + (d_c - left)
            p = source[t, here] if first else pri[t, here]
            g, f = img[t, here], fid[t, here]
            u = (p + (tau_step * sigma_step) * div + f * g) * inv[t, here]
            if final:
                slots_of(start)[:, t * TW:(t + 1) * TW] = u
            else:
                ext[t, here] = u + (u - p)
                pri[t, here] = u
            miss = u - g
            return f * (miss * miss)

        def counted(value):
            if start < 0:
                return jnp.where(sub >= -start, value, 0.0)
            if start + BR > rows:
                return jnp.where(sub < rows - start, value, 0.0)
            return value

        fit, tv = acc
        end = lane == TW - 1
        inner = part in ("inner", "above")
        if not inner:
            turned_halo = ahead(tiles)
            _, h_r, h_c = duals(tiles, jnp.where(end, ahead(0), turned_halo))
            shifted_halo = pltpu.roll(h_c, 1, 1)
            shifted = shifted_halo
        if part == "outer":
            t = tiles - 1
            loss = update(0, dual_r[0, here], dual_c[0, here],
                          jnp.where(lane == 0, shifted_halo, pltpu.roll(dual_c[0, here], 1, 1)))
            steep, d_r, d_c = duals(t, jnp.where(end, turned_halo, ahead(t)))
            shifted = pltpu.roll(d_c, 1, 1)
            loss += update(t, d_r, d_c, jnp.where(lane == 0, pltpu.roll(dual_c[t - 1, here], 1, 1), shifted))
            fit, tv = fit + loss, tv + steep
        else:
            turned = ahead(0)
            for t in range(tiles - 1 if inner else tiles):
                turned_next = ahead(t + 1) if t < tiles - 1 else turned_halo
                steep, d_r, d_c = duals(t, jnp.where(end, turned_next, turned))
                turned = turned_next
                if part in ("duals", "above"):
                    continue
                shifted_here = pltpu.roll(d_c, 1, 1)
                tv = tv + counted(steep)
                if t or not inner:
                    fit = fit + counted(update(t, d_r, d_c, jnp.where(lane == 0, shifted, shifted_here)))
                shifted = shifted_here
        if not (final or inner or part == "duals"):
            update(tiles, h_r, h_c, jnp.where(lane == 0, shifted, shifted_halo))
        return fit, tv

    return sweep


def first_rows(rows):
    return range(-BR // 2, rows, BR)


def early_kernel(
    tiles, blocks, height, width, weights, image, mask,
    seed, img, fid, inv, ext, pri, dual_r, dual_c, weight, sem,
):
    rows = blocks * BR
    fetch = pltpu.make_async_copy(weights, weight, sem.at[0])
    fetch.start()
    fetch.wait()
    for t in range(tiles):
        for b in range(blocks):
            natural, cols = slice(b * BR, (b + 1) * BR), slice(t * TW, (t + 1) * TW)
            here = slice(PAD + b * BR, PAD + (b + 1) * BR)
            f = tile_fidelity(weight[b, t], mask[natural, cols])
            img[t, here] = image[natural, cols]
            fid[t, here] = f
            inv[t, here] = 1.0 / (1.0 + f)
    sweep = sweeper(tiles, rows, height, width, None, img, fid, inv, ext, pri, dual_r, dual_c)
    zero = jnp.zeros((BR, TW), jnp.float32)
    acc = zero, zero
    first, *inner, last = first_rows(rows)
    sweep(0, first, acc, "above")
    for start in inner:
        acc = sweep(0, start, acc, "inner")
    seed[0], seed[1] = acc


def solve_kernel(
    tiles, blocks, height, width,
    owners, edge_b, edge_a, side_b, side_a, seed, *refs,
):
    slots, partial, img, fid, inv, ext, pri, dual_r, dual_c, owner, staged, sem = refs[7:]
    rows = blocks * BR
    fetch_owner = pltpu.make_async_copy(owners, owner, sem.at[blocks])
    fetch_owner.start()
    own_row, own_col = lax.axis_index(ROWS), lax.axis_index(COLS)
    even_row, even_col = lax.rem(own_row, 2) == 0, lax.rem(own_col, 2) == 0
    lane = lax.broadcasted_iota(jnp.int32, (BR, TW), 1)
    sub = lax.broadcasted_iota(jnp.int32, (BR, TW), 0)

    low, high = slice(PAD - BR, PAD), slice(PAD + rows, PAD + rows + BR)
    for t in range(tiles + 1):
        a, b = edge_a[t], edge_b[t]
        v, w = jnp.where(even_row, b, a), jnp.where(even_row, a, b)
        for at, g, f in (
            (low, jnp.where(sub >= 4, pltpu.roll(v, 4, 0), 0.0), jnp.where(sub >= 4, v, 0.0)),
            (high, jnp.where(sub < 4, w, 0.0), jnp.where(sub < 4, pltpu.roll(w, 4, 0), 0.0)),
        ):
            img[t, at] = g
            fid[t, at] = f
            inv[t, at] = 1.0 / (1.0 + f)
    for b in range(blocks):
        here = slice(PAD + b * BR, PAD + (b + 1) * BR)
        g, f = halo_tile(even_col, side_a, side_b, b)
        img[tiles, here] = g
        fid[tiles, here] = f
        inv[tiles, here] = 1.0 / (1.0 + f)

    def send(b):
        return pltpu.make_async_copy(staged.at[b], slots.at[owner[own_row * blocks + b]], sem.at[b])

    sweep = sweeper(
        tiles, rows, height, width, lambda start: staged.at[start // BR], img, fid, inv, ext, pri, dual_r, dual_c
    )
    zero = jnp.zeros((BR, TW), jnp.float32)
    total = zero
    for k in range(ITERS):
        acc = zero, zero
        if k == 0:
            first, *inner, last = first_rows(rows)
            acc = sweep(k, first, (seed[0], seed[1]))
            for start in inner:
                acc = sweep(k, start, acc, "outer")
            acc = sweep(k, last, acc)
        elif k < ITERS - 1:
            for start in first_rows(rows):
                acc = sweep(k, start, acc)
        else:
            sweep(k, -BR, acc, "duals")
            fetch_owner.wait()
            for b in range(blocks):
                acc = sweep(k, b * BR, acc)
                if b:
                    send(b - 1).start()
        fit, tv = acc
        total = jnp.where(lane == k, jnp.sum((0.5 / tau_step) * fit + tv_weight * tv), total)
    send(blocks - 1).start()
    partial[...] = total
    for b in range(blocks):
        send(b).wait()


def lookup_kernel(blocks, owner, senders):
    own_row = lax.axis_index(ROWS)

    def body(sender, found):
        mine = owner[sender * blocks] == own_row
        for i in range(1, blocks):
            mine |= owner[sender * blocks + i] == own_row
        senders[found] = sender
        return found + mine.astype(jnp.int32)

    lax.fori_loop(0, owner.shape[0] // blocks, body, jnp.int32(0))


def place_kernel(blocks, pixels, senders, arrived, *refs):
    parts, (out, objective, sums, sem) = refs[:-4], refs[-4:]
    copies = [
        pltpu.make_async_copy(arrived.at[senders[k]], out.at[pl.ds(k * BR, BR)], sem.at[k]) for k in range(blocks)
    ]
    for copy in copies:
        copy.start()
    values = [part[...] for part in parts]
    while len(values) > 1:
        values = [a + b for a, b in zip(values[::2], values[1::2])]
    lane = lax.broadcasted_iota(jnp.int32, values[0].shape, 1)
    for k in range(ITERS):
        sums[k] = jnp.sum(jnp.where(lane == k, values[0], 0.0)) / pixels
    copies.append(pltpu.make_async_copy(sums, objective, sem.at[blocks]))
    copies[-1].start()
    for copy in copies:
        copy.wait()


def per_device(image, cloud_mask, tile_weight, owner):
    rows_here, width_here = image.shape
    blocks, tiles = rows_here // BR, width_here // TW
    row_count, col_count = lax.axis_size(ROWS), lax.axis_size(COLS)
    height, width = rows_here * row_count, width_here * col_count
    smem, vmem, hbm, anywhere = (pl.BlockSpec(memory_space=s) for s in (pltpu.SMEM, pltpu.VMEM, pltpu.HBM, pl.ANY))

    def shape(*dims):
        return jax.ShapeDtypeStruct(dims, jnp.float32)

    def work(flops):
        return pl.CostEstimate(flops=flops, bytes_accessed=0, transcendentals=0)

    def swap(array, axis, first):
        pairs = [(i, i + 1) for i in range(first, lax.axis_size(axis) - 1, 2)]
        return lax.ppermute(array, axis, pairs + [(j, i) for i, j in pairs])

    edge = shape(tiles + 1, BR, TW)
    side_b, side_a, up, down = pl.pallas_call(
        functools.partial(sides_kernel, tiles),
        in_specs=[hbm] * 3,
        out_specs=[vmem] * 4,
        out_shape=[shape(BR, TW)] * 2 + [edge] * 2,
        scratch_shapes=[
            pltpu.SMEM(tile_weight.shape, jnp.int32),
            pltpu.VMEM((2, rows_here, TW), jnp.float32),
            pltpu.VMEM((2, rows_here, TW), jnp.int32),
            pltpu.VMEM((2, BR, width_here), jnp.float32),
            pltpu.VMEM((2, BR, width_here), jnp.int32),
            pltpu.SemaphoreType.DMA((9,)),
        ],
        cost_estimate=work(2 * 10**9),
        compiler_params=vmem_grant(53.5),
        name="sides",
    )(pltpu.with_memory_space_constraint(tile_weight, pltpu.HBM), image, cloud_mask)
    side_b, side_a = swap(side_b, COLS, 1), swap(side_a, COLS, 0)
    edge_b_out, edge_a_out = pl.pallas_call(
        functools.partial(corners_kernel, tiles, blocks),
        in_specs=[vmem] * 4,
        out_specs=[vmem] * 2,
        out_shape=[edge] * 2,
        cost_estimate=work(2 * 10**9),
        compiler_params=vmem_grant(2),
        name="corners",
    )(side_b, side_a, up, down)
    edge_b, edge_a = swap(edge_b_out, ROWS, 1), swap(edge_a_out, ROWS, 0)
    deep = shape(tiles + 1, PAD + rows_here + PAD, TW)
    own_image, own_mask, _ = lax.optimization_barrier((image, cloud_mask, edge_b_out))
    seed, *fields = pl.pallas_call(
        functools.partial(early_kernel, tiles, blocks, height, width),
        in_specs=[anywhere] + [vmem] * 2,
        out_specs=[vmem] * 8,
        out_shape=[shape(2, BR, TW)] + [deep] * 7,
        scratch_shapes=[pltpu.SMEM(tile_weight.shape, jnp.int32), pltpu.SemaphoreType.DMA((1,))],
        cost_estimate=work(2 * 10**9),
        compiler_params=vmem_grant(32),
        name="early",
    )(tile_weight, own_image, own_mask)
    slots, partial, *_ = pl.pallas_call(
        functools.partial(solve_kernel, tiles, blocks, height, width),
        in_specs=[anywhere] + [vmem] * 12,
        out_specs=[hbm] + [vmem] * 8,
        out_shape=[shape(row_count, BR, width_here), shape(BR, TW)] + [deep] * 7,
        input_output_aliases={6 + i: 2 + i for i in range(7)},
        scratch_shapes=[pltpu.SMEM(owner.shape, jnp.int32)]
        + [pltpu.VMEM((blocks, BR, width_here), jnp.float32), pltpu.SemaphoreType.DMA((blocks + 1,))],
        compiler_params=vmem_grant(48),
        name="solve",
    )(owner, edge_b, edge_a, side_b, side_a, seed, *fields)
    arrived = lax.all_to_all(slots, ROWS, split_axis=0, concat_axis=0, tiled=True)

    later, _ = lax.optimization_barrier((owner, partial))
    senders = pl.pallas_call(
        functools.partial(lookup_kernel, blocks),
        in_specs=[smem],
        out_specs=smem,
        out_shape=jax.ShapeDtypeStruct((2 * blocks,), jnp.int32),
        compiler_params=vmem_grant(1),
        name="lookup",
    )(later)

    devices = row_count * col_count

    def swapped(array, mask):
        return lax.ppermute(array, (ROWS, COLS), [(i, i ^ mask) for i in range(devices)])

    total = partial[:1]
    for bit in (1 << i for i in range(devices.bit_length() - 1)):
        if bit not in ALONG_Z:
            total = total + swapped(total, bit)
    masks = [0]
    for bit in ALONG_Z:
        masks += [mask | bit for mask in masks]
    parts = [total] + [swapped(total, mask) for mask in masks[1:]]

    solution, objective = pl.pallas_call(
        functools.partial(place_kernel, blocks, height * width),
        in_specs=[smem, anywhere] + [vmem] * len(parts),
        out_specs=[anywhere, anywhere],
        out_shape=[shape(rows_here, width_here), shape(ITERS)],
        scratch_shapes=[pltpu.SMEM((ITERS,), jnp.float32), pltpu.SemaphoreType.DMA((blocks + 1,))],
        compiler_params=vmem_grant(1),
        name="place",
    )(senders, arrived, *parts)
    return solution, objective


def solution(mesh):
    placed = (P(ROWS, COLS), P(ROWS, COLS), P(ROWS, COLS), P())
    return jax.shard_map(per_device, mesh=mesh, in_specs=placed, out_specs=(P(ROWS, COLS), P()), check_vma=False)
```

```python
import functools

import jax
import jax.numpy as jnp
from jax import lax
from jax.experimental import pallas as pl
from jax.experimental.pallas import tpu as pltpu
from jax.sharding import PartitionSpec as P


BR = 8
TW = 128
ITERS = 3
HALF = TW // 2
SIDE = 8
PAD = 16
ROWS, COLS = "rows", "cols"
ALONG_Z = (1, 16, 32)

fidelity_scale = 0.25
tau_step = 0.35
sigma_step = 0.35
tv_weight = 0.3


def vmem_grant(mebibytes):
    return pltpu.CompilerParams(vmem_limit_bytes=int(mebibytes * 2**20))


def tile_fidelity(weight, mask):
    return (tau_step * fidelity_scale * weight.astype(jnp.float32)) * (1 - mask).astype(jnp.float32)


def turned(tile, shift):
    return pltpu.roll(tile, shift % TW, 1) if shift % TW else tile


def sides_kernel(tiles, weights, image, mask, swap_b, swap_a, up, down, weight, img, msk, img_rows, msk_rows, sem):
    rows = image.shape[0]
    blocks = rows // BR
    lane = lax.broadcasted_iota(jnp.int32, (BR, TW), 1)
    sub = lax.broadcasted_iota(jnp.int32, (BR, TW), 0)
    copies = [pltpu.make_async_copy(weights, weight, sem.at[0])]
    for side in range(2):
        column, row = pl.ds(side * (tiles - 1) * TW, TW), pl.ds(side * (rows - BR), BR)
        for source, kept, kept_rows in ((image, img, img_rows), (mask, msk, msk_rows)):
            copies.append(pltpu.make_async_copy(source.at[:, column], kept.at[side], sem.at[len(copies)]))
            copies.append(pltpu.make_async_copy(source.at[row], kept_rows.at[side], sem.at[len(copies)]))
    for copy in copies:
        copy.start()
    for copy in copies:
        copy.wait()
    to_left = to_right = jnp.zeros((BR, TW), jnp.float32)
    for b in range(blocks):
        here = slice(b * BR, (b + 1) * BR)
        at = b * 2 * SIDE
        for shift, value in ((at, img[0, here]), (at + SIDE, tile_fidelity(weight[b, 0], msk[0, here]))):
            to_left = jnp.where((lane >= shift) & (lane < shift + SIDE), turned(value, shift), to_left)
        for shift, value in ((at, img[1, here]), (at + SIDE, tile_fidelity(weight[b, tiles - 1], msk[1, here]))):
            to_right = jnp.where((lane >= shift) & (lane < shift + SIDE), turned(value, shift + SIDE), to_right)
    even = lax.rem(lax.axis_index(COLS), 2) == 0
    swap_a[...] = jnp.where(even, to_right, to_left)
    swap_b[...] = jnp.where(even, to_left, to_right)
    for t in range(tiles):
        cols = slice(t * TW, (t + 1) * TW)
        f = tile_fidelity(weight[0, t], msk_rows[0, :, cols])
        up[t] = jnp.where(sub < 4, img_rows[0, :, cols], pltpu.roll(f, 4, 0))
        f = tile_fidelity(weight[blocks - 1, t], msk_rows[1, :, cols])
        down[t] = jnp.where(sub < 4, pltpu.roll(img_rows[1, :, cols], 4, 0), f)


def halo_tile(even, side_a, side_b, block):
    lane = lax.broadcasted_iota(jnp.int32, (BR, TW), 1)
    a, b = side_a[...], side_b[...]
    right, left = jnp.where(even, a, b), jnp.where(even, b, a)
    at = block * 2 * SIDE

    def spread(at):
        return jnp.where(lane < HALF, turned(right, -at), turned(left, -at - SIDE))

    return spread(at), spread(at + SIDE)


def corners_kernel(tiles, blocks, side_b, side_a, up, down, swap_b, swap_a):
    sub = lax.broadcasted_iota(jnp.int32, (BR, TW), 0)
    even_col = lax.rem(lax.axis_index(COLS), 2) == 0
    even_row = lax.rem(lax.axis_index(ROWS), 2) == 0

    def put(t, top, bottom):
        swap_a[t] = jnp.where(even_row, bottom, top)
        swap_b[t] = jnp.where(even_row, top, bottom)

    for t in range(tiles):
        put(t, up[t], down[t])
    g, f = halo_tile(even_col, side_a, side_b, 0)
    top = jnp.where(sub < 4, g, pltpu.roll(f, 4, 0))
    g, f = halo_tile(even_col, side_a, side_b, blocks - 1)
    put(tiles, top, jnp.where(sub < 4, pltpu.roll(g, 4, 0), f))


def sweeper(tiles, rows, height, width, slots_of, img, fid, inv, ext, pri, dual_r, dual_c):
    own_row, own_col = lax.axis_index(ROWS), lax.axis_index(COLS)
    lane = lax.broadcasted_iota(jnp.int32, (BR, TW), 1)
    sub = lax.broadcasted_iota(jnp.int32, (BR, TW), 0)
    col = own_col * (tiles * TW) + lane
    inner_last = col + (tiles - 1) * TW < width - 1
    halo_col = jnp.where(lane < HALF, col + tiles * TW, col - TW)
    inner_halo = (halo_col >= 0) & (halo_col < width - 1)

    def sweep(k, start, acc, part="all"):
        base = PAD + start
        here, lower, upper = pl.ds(base, BR), pl.ds(base + 1, BR), pl.ds(base - 1, BR)
        first, final = k == 0, k == ITERS - 1
        source = img if first else ext
        row = own_row * rows + start + sub
        inner_row = (row >= 0) & (row < height - 1)

        def ahead(t):
            return pltpu.roll(source[t, here], TW - 1, 1)

        def duals(t, right):
            e = source[t, here]
            g_r = source[t, lower] - e
            if start < 0 or start + BR >= rows:
                g_r = jnp.where(inner_row, g_r, 0.0)
            g_c = right - e
            if t == tiles - 1:
                g_c = jnp.where(inner_last, g_c, 0.0)
            if t == tiles:
                g_c = jnp.where(inner_halo, g_c, 0.0)
            n = g_r * g_r + g_c * g_c
            s = lax.rsqrt(n)
            steep = jnp.where(n > 0.0, n * s, 0.0)
            q_r, q_c = g_r, g_c
            if not first:
                q_r, q_c = dual_r[t, here] + q_r, dual_c[t, here] + q_c
                s = lax.rsqrt(q_r * q_r + q_c * q_c)
            scale = jnp.minimum(1.0, (tv_weight / sigma_step) * s)
            d_r, d_c = q_r * scale, q_c * scale
            dual_r[t, here] = d_r
            if not final:
                dual_c[t, here] = d_c
            return steep, d_r, d_c

        def update(t, d_r, d_c, left):
            div = d_r - dual_r[t, upper] + (d_c - left)
            p = source[t, here] if first else pri[t, here]
            g, f = img[t, here], fid[t, here]
            u = (p + (tau_step * sigma_step) * div + f * g) * inv[t, here]
            if final:
                slots_of(start)[:, t * TW:(t + 1) * TW] = u
            else:
                ext[t, here] = u + (u - p)
                pri[t, here] = u
            miss = u - g
            return f * (miss * miss)

        def counted(value):
            if start < 0:
                return jnp.where(sub >= -start, value, 0.0)
            if start + BR > rows:
                return jnp.where(sub < rows - start, value, 0.0)
            return value

        fit, tv = acc
        end = lane == TW - 1
        inner = part in ("inner", "above")
        if not inner:
            turned_halo = ahead(tiles)
            _, h_r, h_c = duals(tiles, jnp.where(end, ahead(0), turned_halo))
            shifted_halo = pltpu.roll(h_c, 1, 1)
            shifted = shifted_halo
        if part == "outer":
            t = tiles - 1
            loss = update(0, dual_r[0, here], dual_c[0, here],
                          jnp.where(lane == 0, shifted_halo, pltpu.roll(dual_c[0, here], 1, 1)))
            steep, d_r, d_c = duals(t, jnp.where(end, turned_halo, ahead(t)))
            shifted = pltpu.roll(d_c, 1, 1)
            loss += update(t, d_r, d_c, jnp.where(lane == 0, pltpu.roll(dual_c[t - 1, here], 1, 1), shifted))
            fit, tv = fit + loss, tv + steep
        else:
            turned = ahead(0)
            for t in range(tiles - 1 if inner else tiles):
                turned_next = ahead(t + 1) if t < tiles - 1 else turned_halo
                steep, d_r, d_c = duals(t, jnp.where(end, turned_next, turned))
                turned = turned_next
                if part in ("duals", "above"):
                    continue
                shifted_here = pltpu.roll(d_c, 1, 1)
                tv = tv + counted(steep)
                if t or not inner:
                    fit = fit + counted(update(t, d_r, d_c, jnp.where(lane == 0, shifted, shifted_here)))
                shifted = shifted_here
        if not (final or inner or part == "duals"):
            update(tiles, h_r, h_c, jnp.where(lane == 0, shifted, shifted_halo))
        return fit, tv

    return sweep


def first_rows(rows):
    return range(-BR // 2, rows, BR)


def early_kernel(
    tiles, blocks, height, width, weights, image, mask,
    seed, img, fid, inv, ext, pri, dual_r, dual_c, weight, sem,
):
    rows = blocks * BR
    fetch = pltpu.make_async_copy(weights, weight, sem.at[0])
    fetch.start()
    fetch.wait()
    for t in range(tiles):
        for b in range(blocks):
            natural, cols = slice(b * BR, (b + 1) * BR), slice(t * TW, (t + 1) * TW)
            here = slice(PAD + b * BR, PAD + (b + 1) * BR)
            f = tile_fidelity(weight[b, t], mask[natural, cols])
            img[t, here] = image[natural, cols]
            fid[t, here] = f
            inv[t, here] = 1.0 / (1.0 + f)
    sweep = sweeper(tiles, rows, height, width, None, img, fid, inv, ext, pri, dual_r, dual_c)
    zero = jnp.zeros((BR, TW), jnp.float32)
    acc = zero, zero
    first, *inner, last = first_rows(rows)
    sweep(0, first, acc, "above")
    for start in inner:
        acc = sweep(0, start, acc, "inner")
    seed[0], seed[1] = acc


def solve_kernel(
    tiles, blocks, height, width,
    owners, edge_b, edge_a, side_b, side_a, seed, *refs,
):
    slots, partial, img, fid, inv, ext, pri, dual_r, dual_c, owner, staged, sem = refs[7:]
    rows = blocks * BR
    fetch_owner = pltpu.make_async_copy(owners, owner, sem.at[blocks])
    fetch_owner.start()
    own_row, own_col = lax.axis_index(ROWS), lax.axis_index(COLS)
    even_row, even_col = lax.rem(own_row, 2) == 0, lax.rem(own_col, 2) == 0
    lane = lax.broadcasted_iota(jnp.int32, (BR, TW), 1)
    sub = lax.broadcasted_iota(jnp.int32, (BR, TW), 0)

    low, high = slice(PAD - BR, PAD), slice(PAD + rows, PAD + rows + BR)
    for t in range(tiles + 1):
        a, b = edge_a[t], edge_b[t]
        v, w = jnp.where(even_row, b, a), jnp.where(even_row, a, b)
        for at, g, f in (
            (low, jnp.where(sub >= 4, pltpu.roll(v, 4, 0), 0.0), jnp.where(sub >= 4, v, 0.0)),
            (high, jnp.where(sub < 4, w, 0.0), jnp.where(sub < 4, pltpu.roll(w, 4, 0), 0.0)),
        ):
            img[t, at] = g
            fid[t, at] = f
            inv[t, at] = 1.0 / (1.0 + f)
    for b in range(blocks):
        here = slice(PAD + b * BR, PAD + (b + 1) * BR)
        g, f = halo_tile(even_col, side_a, side_b, b)
        img[tiles, here] = g
        fid[tiles, here] = f
        inv[tiles, here] = 1.0 / (1.0 + f)

    def send(b):
        return pltpu.make_async_copy(staged.at[b], slots.at[owner[own_row * blocks + b]], sem.at[b])

    sweep = sweeper(
        tiles, rows, height, width, lambda start: staged.at[start // BR], img, fid, inv, ext, pri, dual_r, dual_c
    )
    zero = jnp.zeros((BR, TW), jnp.float32)
    total = zero
    for k in range(ITERS):
        acc = zero, zero
        if k == 0:
            first, *inner, last = first_rows(rows)
            acc = sweep(k, first, (seed[0], seed[1]))
            for start in inner:
                acc = sweep(k, start, acc, "outer")
            acc = sweep(k, last, acc)
        elif k < ITERS - 1:
            for start in first_rows(rows):
                acc = sweep(k, start, acc)
        else:
            sweep(k, -BR, acc, "duals")
            fetch_owner.wait()
            for b in range(blocks):
                acc = sweep(k, b * BR, acc)
                if b:
                    send(b - 1).start()
        fit, tv = acc
        total = jnp.where(lane == k, jnp.sum((0.5 / tau_step) * fit + tv_weight * tv), total)
    send(blocks - 1).start()
    partial[...] = total
    for b in range(blocks):
        send(b).wait()


def lookup_kernel(blocks, owner, senders):
    own_row = lax.axis_index(ROWS)

    def body(sender, found):
        mine = owner[sender * blocks] == own_row
        for i in range(1, blocks):
            mine |= owner[sender * blocks + i] == own_row
        senders[found] = sender
        return found + mine.astype(jnp.int32)

    lax.fori_loop(0, owner.shape[0] // blocks, body, jnp.int32(0))


def place_kernel(blocks, senders, arrived, out, sem):
    copies = [
        pltpu.make_async_copy(arrived.at[senders[k]], out.at[pl.ds(k * BR, BR)], sem.at[k]) for k in range(blocks)
    ]
    for copy in copies:
        copy.start()
    for copy in copies:
        copy.wait()


def combine_kernel(pixels, *refs):
    parts, objective = refs[:-1], refs[-1]
    values = [part[...] for part in parts]
    while len(values) > 1:
        values = [a + b for a, b in zip(values[::2], values[1::2])]
    lane = lax.broadcasted_iota(jnp.int32, values[0].shape, 1)
    for k in range(ITERS):
        objective[k] = jnp.sum(jnp.where(lane == k, values[0], 0.0)) / pixels


def per_device(image, cloud_mask, tile_weight, owner):
    rows_here, width_here = image.shape
    blocks, tiles = rows_here // BR, width_here // TW
    row_count, col_count = lax.axis_size(ROWS), lax.axis_size(COLS)
    height, width = rows_here * row_count, width_here * col_count
    smem, vmem, hbm, anywhere = (pl.BlockSpec(memory_space=s) for s in (pltpu.SMEM, pltpu.VMEM, pltpu.HBM, pl.ANY))

    def shape(*dims):
        return jax.ShapeDtypeStruct(dims, jnp.float32)

    def work(flops):
        return pl.CostEstimate(flops=flops, bytes_accessed=0, transcendentals=0)

    def swap(array, axis, first):
        pairs = [(i, i + 1) for i in range(first, lax.axis_size(axis) - 1, 2)]
        return lax.ppermute(array, axis, pairs + [(j, i) for i, j in pairs])

    edge = shape(tiles + 1, BR, TW)
    side_b, side_a, up, down = pl.pallas_call(
        functools.partial(sides_kernel, tiles),
        in_specs=[hbm] * 3,
        out_specs=[vmem] * 4,
        out_shape=[shape(BR, TW)] * 2 + [edge] * 2,
        scratch_shapes=[
            pltpu.SMEM(tile_weight.shape, jnp.int32),
            pltpu.VMEM((2, rows_here, TW), jnp.float32),
            pltpu.VMEM((2, rows_here, TW), jnp.int32),
            pltpu.VMEM((2, BR, width_here), jnp.float32),
            pltpu.VMEM((2, BR, width_here), jnp.int32),
            pltpu.SemaphoreType.DMA((9,)),
        ],
        cost_estimate=work(2 * 10**9),
        compiler_params=vmem_grant(53.5),
        name="sides",
    )(pltpu.with_memory_space_constraint(tile_weight, pltpu.HBM), image, cloud_mask)
    side_b, side_a = swap(side_b, COLS, 1), swap(side_a, COLS, 0)
    edge_b_out, edge_a_out = pl.pallas_call(
        functools.partial(corners_kernel, tiles, blocks),
        in_specs=[vmem] * 4,
        out_specs=[vmem] * 2,
        out_shape=[edge] * 2,
        cost_estimate=work(2 * 10**9),
        compiler_params=vmem_grant(2),
        name="corners",
    )(side_b, side_a, up, down)
    edge_b, edge_a = swap(edge_b_out, ROWS, 1), swap(edge_a_out, ROWS, 0)
    deep = shape(tiles + 1, PAD + rows_here + PAD, TW)
    own_image, own_mask, _ = lax.optimization_barrier((image, cloud_mask, edge_b_out))
    seed, *fields = pl.pallas_call(
        functools.partial(early_kernel, tiles, blocks, height, width),
        in_specs=[anywhere] + [vmem] * 2,
        out_specs=[vmem] * 8,
        out_shape=[shape(2, BR, TW)] + [deep] * 7,
        scratch_shapes=[pltpu.SMEM(tile_weight.shape, jnp.int32), pltpu.SemaphoreType.DMA((1,))],
        cost_estimate=work(2 * 10**9),
        compiler_params=vmem_grant(32),
        name="early",
    )(tile_weight, own_image, own_mask)
    slots, partial, *_ = pl.pallas_call(
        functools.partial(solve_kernel, tiles, blocks, height, width),
        in_specs=[anywhere] + [vmem] * 12,
        out_specs=[hbm] + [vmem] * 8,
        out_shape=[shape(row_count, BR, width_here), shape(BR, TW)] + [deep] * 7,
        input_output_aliases={6 + i: 2 + i for i in range(7)},
        scratch_shapes=[pltpu.SMEM(owner.shape, jnp.int32)]
        + [pltpu.VMEM((blocks, BR, width_here), jnp.float32), pltpu.SemaphoreType.DMA((blocks + 1,))],
        compiler_params=vmem_grant(48),
        name="solve",
    )(owner, edge_b, edge_a, side_b, side_a, seed, *fields)
    arrived = lax.all_to_all(slots, ROWS, split_axis=0, concat_axis=0, tiled=True)

    later, _ = lax.optimization_barrier((owner, partial))
    senders = pl.pallas_call(
        functools.partial(lookup_kernel, blocks),
        in_specs=[smem],
        out_specs=smem,
        out_shape=jax.ShapeDtypeStruct((2 * blocks,), jnp.int32),
        compiler_params=vmem_grant(1),
        name="lookup",
    )(later)

    devices = row_count * col_count

    def swapped(array, mask):
        return lax.ppermute(array, (ROWS, COLS), [(i, i ^ mask) for i in range(devices)])

    total = partial[:1]
    for bit in (1 << i for i in range(devices.bit_length() - 1)):
        if bit not in ALONG_Z:
            total = total + swapped(total, bit)
    masks = [0]
    for bit in ALONG_Z:
        masks += [mask | bit for mask in masks]
    parts = [total] + [swapped(total, mask) for mask in masks[1:]]

    solution = pl.pallas_call(
        functools.partial(place_kernel, blocks),
        in_specs=[smem, anywhere],
        out_specs=anywhere,
        out_shape=shape(rows_here, width_here),
        scratch_shapes=[pltpu.SemaphoreType.DMA((blocks,))],
        compiler_params=vmem_grant(1),
        name="place",
    )(senders, arrived)
    objective = pl.pallas_call(
        functools.partial(combine_kernel, height * width),
        in_specs=[vmem] * len(parts),
        out_specs=smem,
        out_shape=shape(ITERS),
        compiler_params=vmem_grant(1),
        name="combine",
    )(*parts)
    return solution, objective


def solution(mesh):
    placed = (P(ROWS, COLS), P(ROWS, COLS), P(ROWS, COLS), P())
    return jax.shard_map(per_device, mesh=mesh, in_specs=placed, out_specs=(P(ROWS, COLS), P()), check_vma=False)
```

```python
import functools

import jax
import jax.numpy as jnp
from jax import lax
from jax.experimental import pallas as pl
from jax.experimental.pallas import tpu as pltpu
from jax.sharding import PartitionSpec as P

BR = 8
TW = 128
ITERS = 3
HALF = TW // 2
SIDE = 8
PAD = 16
ROWS, COLS = "rows", "cols"
ALONG_Z = (1, 16, 32)

fidelity_scale = 0.25
tau_step = 0.35
sigma_step = 0.35
tv_weight = 0.3


def vmem_grant(mebibytes):
    return pltpu.CompilerParams(vmem_limit_bytes=int(mebibytes * 2**20))


def tile_fidelity(weight, mask):
    return (tau_step * fidelity_scale * weight.astype(jnp.float32)) * (1 - mask).astype(jnp.float32)


def turned(tile, shift):
    return pltpu.roll(tile, shift % TW, 1) if shift % TW else tile


def sides_kernel(tiles, weights, image, mask, swap_b, swap_a, up, down, weight, img, msk, img_rows, msk_rows, sem):
    rows = image.shape[0]
    blocks = rows // BR
    lane = lax.broadcasted_iota(jnp.int32, (BR, TW), 1)
    sub = lax.broadcasted_iota(jnp.int32, (BR, TW), 0)
    copies = [pltpu.make_async_copy(weights, weight, sem.at[0])]
    for side in range(2):
        column, row = pl.ds(side * (tiles - 1) * TW, TW), pl.ds(side * (rows - BR), BR)
        for source, kept, kept_rows in ((image, img, img_rows), (mask, msk, msk_rows)):
            copies.append(pltpu.make_async_copy(source.at[:, column], kept.at[side], sem.at[len(copies)]))
            copies.append(pltpu.make_async_copy(source.at[row], kept_rows.at[side], sem.at[len(copies)]))
    for copy in copies:
        copy.start()
    for copy in copies:
        copy.wait()
    to_left = to_right = jnp.zeros((BR, TW), jnp.float32)
    for b in range(blocks):
        here = slice(b * BR, (b + 1) * BR)
        at = b * 2 * SIDE
        for shift, value in ((at, img[0, here]), (at + SIDE, tile_fidelity(weight[b, 0], msk[0, here]))):
            to_left = jnp.where((lane >= shift) & (lane < shift + SIDE), turned(value, shift), to_left)
        for shift, value in ((at, img[1, here]), (at + SIDE, tile_fidelity(weight[b, tiles - 1], msk[1, here]))):
            to_right = jnp.where((lane >= shift) & (lane < shift + SIDE), turned(value, shift + SIDE), to_right)
    even = lax.rem(lax.axis_index(COLS), 2) == 0
    swap_a[...] = jnp.where(even, to_right, to_left)
    swap_b[...] = jnp.where(even, to_left, to_right)
    for t in range(tiles):
        cols = slice(t * TW, (t + 1) * TW)
        f = tile_fidelity(weight[0, t], msk_rows[0, :, cols])
        up[t] = jnp.where(sub < 4, img_rows[0, :, cols], pltpu.roll(f, 4, 0))
        f = tile_fidelity(weight[blocks - 1, t], msk_rows[1, :, cols])
        down[t] = jnp.where(sub < 4, pltpu.roll(img_rows[1, :, cols], 4, 0), f)


def halo_tile(even, side_a, side_b, block):
    lane = lax.broadcasted_iota(jnp.int32, (BR, TW), 1)
    a, b = side_a[...], side_b[...]
    right, left = jnp.where(even, a, b), jnp.where(even, b, a)
    at = block * 2 * SIDE

    def spread(at):
        return jnp.where(lane < HALF, turned(right, -at), turned(left, -at - SIDE))

    return spread(at), spread(at + SIDE)


def corners_kernel(tiles, blocks, side_b, side_a, up, down, swap_b, swap_a):
    sub = lax.broadcasted_iota(jnp.int32, (BR, TW), 0)
    even_col = lax.rem(lax.axis_index(COLS), 2) == 0
    even_row = lax.rem(lax.axis_index(ROWS), 2) == 0

    def put(t, top, bottom):
        swap_a[t] = jnp.where(even_row, bottom, top)
        swap_b[t] = jnp.where(even_row, top, bottom)

    for t in range(tiles):
        put(t, up[t], down[t])
    g, f = halo_tile(even_col, side_a, side_b, 0)
    top = jnp.where(sub < 4, g, pltpu.roll(f, 4, 0))
    g, f = halo_tile(even_col, side_a, side_b, blocks - 1)
    put(tiles, top, jnp.where(sub < 4, pltpu.roll(g, 4, 0), f))


def sweeper(tiles, rows, height, width, slots_of, img, fid, inv, ext, pri, dual_r, dual_c):
    own_row, own_col = lax.axis_index(ROWS), lax.axis_index(COLS)
    lane = lax.broadcasted_iota(jnp.int32, (BR, TW), 1)
    sub = lax.broadcasted_iota(jnp.int32, (BR, TW), 0)
    col = own_col * (tiles * TW) + lane
    inner_last = col + (tiles - 1) * TW < width - 1
    halo_col = jnp.where(lane < HALF, col + tiles * TW, col - TW)
    inner_halo = (halo_col >= 0) & (halo_col < width - 1)

    def sweep(k, start, acc, part="all"):
        base = PAD + start
        here, lower, upper = pl.ds(base, BR), pl.ds(base + 1, BR), pl.ds(base - 1, BR)
        first, final = k == 0, k == ITERS - 1
        source = img if first else ext
        row = own_row * rows + start + sub
        inner_row = (row >= 0) & (row < height - 1)

        def ahead(t):
            return pltpu.roll(source[t, here], TW - 1, 1)

        def duals(t, right):
            e = source[t, here]
            g_r = source[t, lower] - e
            if start < 0 or start + BR >= rows:
                g_r = jnp.where(inner_row, g_r, 0.0)
            g_c = right - e
            if t == tiles - 1:
                g_c = jnp.where(inner_last, g_c, 0.0)
            if t == tiles:
                g_c = jnp.where(inner_halo, g_c, 0.0)
            n = g_r * g_r + g_c * g_c
            s = lax.rsqrt(n)
            steep = jnp.where(n > 0.0, n * s, 0.0)
            q_r, q_c = g_r, g_c
            if not first:
                q_r, q_c = dual_r[t, here] + q_r, dual_c[t, here] + q_c
                s = lax.rsqrt(q_r * q_r + q_c * q_c)
            scale = jnp.minimum(1.0, (tv_weight / sigma_step) * s)
            d_r, d_c = q_r * scale, q_c * scale
            dual_r[t, here] = d_r
            if not final:
                dual_c[t, here] = d_c
            return steep, d_r, d_c

        def update(t, d_r, d_c, left):
            div = d_r - dual_r[t, upper] + (d_c - left)
            p = source[t, here] if first else pri[t, here]
            g, f = img[t, here], fid[t, here]
            u = (p + (tau_step * sigma_step) * div + f * g) * inv[t, here]
            if final:
                slots_of(start)[:, t * TW:(t + 1) * TW] = u
            else:
                ext[t, here] = u + (u - p)
                pri[t, here] = u
            miss = u - g
            return f * (miss * miss)

        def counted(value):
            if start < 0:
                return jnp.where(sub >= -start, value, 0.0)
            if start + BR > rows:
                return jnp.where(sub < rows - start, value, 0.0)
            return value

        fit, tv = acc
        end = lane == TW - 1
        inner = part in ("inner", "above")
        if not inner:
            turned_halo = ahead(tiles)
            _, h_r, h_c = duals(tiles, jnp.where(end, ahead(0), turned_halo))
            shifted_halo = pltpu.roll(h_c, 1, 1)
            shifted = shifted_halo
        if part == "outer":
            t = tiles - 1
            loss = update(0, dual_r[0, here], dual_c[0, here],
                          jnp.where(lane == 0, shifted_halo, pltpu.roll(dual_c[0, here], 1, 1)))
            steep, d_r, d_c = duals(t, jnp.where(end, turned_halo, ahead(t)))
            shifted = pltpu.roll(d_c, 1, 1)
            loss += update(t, d_r, d_c, jnp.where(lane == 0, pltpu.roll(dual_c[t - 1, here], 1, 1), shifted))
            fit, tv = fit + loss, tv + steep
        else:
            turned = ahead(0)
            for t in range(tiles - 1 if inner else tiles):
                turned_next = ahead(t + 1) if t < tiles - 1 else turned_halo
                steep, d_r, d_c = duals(t, jnp.where(end, turned_next, turned))
                turned = turned_next
                if part in ("duals", "above"):
                    continue
                shifted_here = pltpu.roll(d_c, 1, 1)
                tv = tv + counted(steep)
                if t or not inner:
                    fit = fit + counted(update(t, d_r, d_c, jnp.where(lane == 0, shifted, shifted_here)))
                shifted = shifted_here
        if not (final or inner or part == "duals"):
            update(tiles, h_r, h_c, jnp.where(lane == 0, shifted, shifted_halo))
        return fit, tv

    return sweep


def first_rows(rows):
    return range(-BR // 2, rows, BR)


def early_kernel(
    tiles, blocks, height, width, weights, image, mask,
    seed, img, fid, inv, ext, pri, dual_r, dual_c, weight, sem,
):
    rows = blocks * BR
    fetch = pltpu.make_async_copy(weights, weight, sem.at[0])
    fetch.start()
    fetch.wait()
    for t in range(tiles):
        for b in range(blocks):
            natural, cols = slice(b * BR, (b + 1) * BR), slice(t * TW, (t + 1) * TW)
            here = slice(PAD + b * BR, PAD + (b + 1) * BR)
            f = tile_fidelity(weight[b, t], mask[natural, cols])
            img[t, here] = image[natural, cols]
            fid[t, here] = f
            inv[t, here] = 1.0 / (1.0 + f)
    sweep = sweeper(tiles, rows, height, width, None, img, fid, inv, ext, pri, dual_r, dual_c)
    zero = jnp.zeros((BR, TW), jnp.float32)
    acc = zero, zero
    first, *inner, last = first_rows(rows)
    sweep(0, first, acc, "above")
    for start in inner:
        acc = sweep(0, start, acc, "inner")
    seed[0], seed[1] = acc


def solve_kernel(
    tiles, blocks, height, width,
    owners, edge_b, edge_a, side_b, side_a, seed, *refs,
):
    slots, partial, img, fid, inv, ext, pri, dual_r, dual_c, owner, staged, sem = refs[7:]
    rows = blocks * BR
    fetch_owner = pltpu.make_async_copy(owners, owner, sem.at[blocks])
    fetch_owner.start()
    own_row, own_col = lax.axis_index(ROWS), lax.axis_index(COLS)
    even_row, even_col = lax.rem(own_row, 2) == 0, lax.rem(own_col, 2) == 0
    lane = lax.broadcasted_iota(jnp.int32, (BR, TW), 1)
    sub = lax.broadcasted_iota(jnp.int32, (BR, TW), 0)

    low, high = slice(PAD - BR, PAD), slice(PAD + rows, PAD + rows + BR)
    for t in range(tiles + 1):
        a, b = edge_a[t], edge_b[t]
        v, w = jnp.where(even_row, b, a), jnp.where(even_row, a, b)
        for at, g, f in (
            (low, jnp.where(sub >= 4, pltpu.roll(v, 4, 0), 0.0), jnp.where(sub >= 4, v, 0.0)),
            (high, jnp.where(sub < 4, w, 0.0), jnp.where(sub < 4, pltpu.roll(w, 4, 0), 0.0)),
        ):
            img[t, at] = g
            fid[t, at] = f
            inv[t, at] = 1.0 / (1.0 + f)
    for b in range(blocks):
        here = slice(PAD + b * BR, PAD + (b + 1) * BR)
        g, f = halo_tile(even_col, side_a, side_b, b)
        img[tiles, here] = g
        fid[tiles, here] = f
        inv[tiles, here] = 1.0 / (1.0 + f)

    def send(b):
        return pltpu.make_async_copy(staged.at[b], slots.at[owner[own_row * blocks + b]], sem.at[b])

    sweep = sweeper(
        tiles, rows, height, width, lambda start: staged.at[start // BR], img, fid, inv, ext, pri, dual_r, dual_c
    )
    zero = jnp.zeros((BR, TW), jnp.float32)
    total = zero
    for k in range(ITERS):
        acc = zero, zero
        if k == 0:
            first, *inner, last = first_rows(rows)
            acc = sweep(k, first, (seed[0], seed[1]))
            for start in inner:
                acc = sweep(k, start, acc, "outer")
            acc = sweep(k, last, acc)
        elif k < ITERS - 1:
            for start in first_rows(rows):
                acc = sweep(k, start, acc)
        else:
            sweep(k, -BR, acc, "duals")
            fetch_owner.wait()
            for b in range(blocks):
                acc = sweep(k, b * BR, acc)
                if b:
                    send(b - 1).start()
        fit, tv = acc
        total = jnp.where(lane == k, jnp.sum((0.5 / tau_step) * fit + tv_weight * tv), total)
    send(blocks - 1).start()
    partial[...] = total
    for b in range(blocks):
        send(b).wait()


def lookup_kernel(blocks, owner, senders):
    own_row = lax.axis_index(ROWS)

    def body(sender, found):
        mine = owner[sender * blocks] == own_row
        for i in range(1, blocks):
            mine |= owner[sender * blocks + i] == own_row
        senders[found] = sender
        return found + mine.astype(jnp.int32)

    lax.fori_loop(0, owner.shape[0] // blocks, body, jnp.int32(0))


def place_kernel(blocks, pixels, senders, arrived, *refs):
    parts, (out, objective, sums, sem) = refs[:-4], refs[-4:]
    copies = [
        pltpu.make_async_copy(arrived.at[senders[k]], out.at[pl.ds(k * BR, BR)], sem.at[k]) for k in range(blocks)
    ]
    for copy in copies:
        copy.start()
    values = [part[...] for part in parts]
    while len(values) > 1:
        values = [a + b for a, b in zip(values[::2], values[1::2])]
    lane = lax.broadcasted_iota(jnp.int32, values[0].shape, 1)
    for k in range(ITERS):
        sums[k] = jnp.sum(jnp.where(lane == k, values[0], 0.0)) / pixels
    copies.append(pltpu.make_async_copy(sums, objective, sem.at[blocks]))
    copies[-1].start()
    for copy in copies:
        copy.wait()


def per_device(image, cloud_mask, tile_weight, owner):
    rows_here, width_here = image.shape
    blocks, tiles = rows_here // BR, width_here // TW
    row_count, col_count = lax.axis_size(ROWS), lax.axis_size(COLS)
    height, width = rows_here * row_count, width_here * col_count
    smem, vmem, hbm, anywhere = (pl.BlockSpec(memory_space=s) for s in (pltpu.SMEM, pltpu.VMEM, pltpu.HBM, pl.ANY))

    def shape(*dims):
        return jax.ShapeDtypeStruct(dims, jnp.float32)

    def work(flops):
        return pl.CostEstimate(flops=flops, bytes_accessed=0, transcendentals=0)

    def swap(array, axis, first):
        pairs = [(i, i + 1) for i in range(first, lax.axis_size(axis) - 1, 2)]
        return lax.ppermute(array, axis, pairs + [(j, i) for i, j in pairs])

    edge = shape(tiles + 1, BR, TW)
    side_b, side_a, up, down = pl.pallas_call(
        functools.partial(sides_kernel, tiles),
        in_specs=[hbm] * 3,
        out_specs=[vmem] * 4,
        out_shape=[shape(BR, TW)] * 2 + [edge] * 2,
        scratch_shapes=[
            pltpu.SMEM(tile_weight.shape, jnp.int32),
            pltpu.VMEM((2, rows_here, TW), jnp.float32),
            pltpu.VMEM((2, rows_here, TW), jnp.int32),
            pltpu.VMEM((2, BR, width_here), jnp.float32),
            pltpu.VMEM((2, BR, width_here), jnp.int32),
            pltpu.SemaphoreType.DMA((9,)),
        ],
        cost_estimate=work(2 * 10**9),
        compiler_params=vmem_grant(53.5),
        name="sides",
    )(pltpu.with_memory_space_constraint(tile_weight, pltpu.HBM), image, cloud_mask)
    side_b, side_a = swap(side_b, COLS, 1), swap(side_a, COLS, 0)
    edge_b_out, edge_a_out = pl.pallas_call(
        functools.partial(corners_kernel, tiles, blocks),
        in_specs=[vmem] * 4,
        out_specs=[vmem] * 2,
        out_shape=[edge] * 2,
        cost_estimate=work(2 * 10**9),
        compiler_params=vmem_grant(2),
        name="corners",
    )(side_b, side_a, up, down)
    edge_b, edge_a = swap(edge_b_out, ROWS, 1), swap(edge_a_out, ROWS, 0)
    deep = shape(tiles + 1, PAD + rows_here + PAD + BR, TW)
    own_image, own_mask, _ = lax.optimization_barrier((image, cloud_mask, edge_b_out))
    seed, *fields = pl.pallas_call(
        functools.partial(early_kernel, tiles, blocks, height, width),
        in_specs=[anywhere] + [vmem] * 2,
        out_specs=[vmem] * 8,
        out_shape=[shape(2, BR, TW)] + [deep] * 7,
        scratch_shapes=[pltpu.SMEM(tile_weight.shape, jnp.int32), pltpu.SemaphoreType.DMA((1,))],
        cost_estimate=work(2 * 10**9),
        compiler_params=vmem_grant(32),
        name="early",
    )(tile_weight, own_image, own_mask)
    slots, partial, *_ = pl.pallas_call(
        functools.partial(solve_kernel, tiles, blocks, height, width),
        in_specs=[anywhere] + [vmem] * 12,
        out_specs=[hbm] + [vmem] * 8,
        out_shape=[shape(row_count, BR, width_here), shape(BR, TW)] + [deep] * 7,
        input_output_aliases={6 + i: 2 + i for i in range(7)},
        scratch_shapes=[pltpu.SMEM(owner.shape, jnp.int32)]
        + [pltpu.VMEM((blocks, BR, width_here), jnp.float32), pltpu.SemaphoreType.DMA((blocks + 1,))],
        compiler_params=vmem_grant(47.5),
        name="solve",
    )(owner, edge_b, edge_a, side_b, side_a, seed, *fields)
    arrived = lax.all_to_all(slots, ROWS, split_axis=0, concat_axis=0, tiled=True)

    later, _ = lax.optimization_barrier((owner, partial))
    senders = pl.pallas_call(
        functools.partial(lookup_kernel, blocks),
        in_specs=[smem],
        out_specs=smem,
        out_shape=jax.ShapeDtypeStruct((2 * blocks,), jnp.int32),
        compiler_params=vmem_grant(1),
        name="lookup",
    )(later)

    devices = row_count * col_count

    def swapped(array, mask):
        return lax.ppermute(array, (ROWS, COLS), [(i, i ^ mask) for i in range(devices)])

    total = partial[:1]
    for bit in (1 << i for i in range(devices.bit_length() - 1)):
        if bit not in ALONG_Z:
            total = total + swapped(total, bit)
    masks = [0]
    for bit in ALONG_Z:
        masks += [mask | bit for mask in masks]
    parts = [total] + [swapped(total, mask) for mask in masks[1:]]

    solution, objective = pl.pallas_call(
        functools.partial(place_kernel, blocks, height * width),
        in_specs=[smem, anywhere] + [vmem] * len(parts),
        out_specs=[anywhere, anywhere],
        out_shape=[shape(rows_here, width_here), shape(ITERS)],
        scratch_shapes=[pltpu.SMEM((ITERS,), jnp.float32), pltpu.SemaphoreType.DMA((blocks + 1,))],
        compiler_params=vmem_grant(1),
        name="place",
    )(senders, arrived, *parts)
    return solution, objective


def solution(mesh):
    placed = (P(ROWS, COLS), P(ROWS, COLS), P(ROWS, COLS), P())
    return jax.shard_map(per_device, mesh=mesh, in_specs=placed, out_specs=(P(ROWS, COLS), P()), check_vma=False)
```
